128 devices in a mesh: dp: 1, dcp: 128 (over z, y, x, core).
Axes of the slice: x: 4, y: 4, z: 4, core: 2. Of those that a mesh axis runs over, the one named last changes fastest.
Arguments:
- q_abs: bfloat16 [64, 2, 128, 576], P('dp', None, 'dcp')
- kv_cache: bfloat16 [64, 2, 128, 64, 576], P('dp', None, 'dcp')
- lengths: int32 [64], P('dp')
Outputs:
- output: bfloat16 [64, 2, 128, 512], P('dp', None, 'dcp')
All inputs are finite; a program needn't handle non-finite values.
Results may differ from the reference program's by a relative error of at most 0.00650124.
Values are sent between devices in bfloat16 or wider.
A program may use at most 1 GiB of HBM per device.

```python
import math
import jax
import jax.numpy as jnp
from jax import lax

BATCH = 64
MTP = 2
HEADS = 128
LATENT = 512
ROPE = 64
NOPE = 128
ROUNDS = 2
GROUP = 128
PAGE = 64

SEQ = ROUNDS * GROUP * PAGE
WIDTH = LATENT + ROPE


def setup_inputs(seed: int = 0, part: int = 0) -> dict:
    base_key = jax.random.fold_in(jax.random.key(seed), part)
    key_qlat, key_qrope, key_cache, key_len, key_pick = jax.random.split(base_key, 5)
    lat_scale = math.sqrt(SEQ / 256.0)
    q_lat = jax.random.normal(key_qlat, (BATCH, MTP, HEADS, LATENT), jnp.float32) * (math.sqrt(1.8 * (NOPE + ROPE) / LATENT) / lat_scale)
    q_rope = jax.random.normal(key_qrope, (BATCH, MTP, HEADS, ROPE), jnp.float32) * math.sqrt(1.8 * (NOPE + ROPE) / ROPE)
    q_abs = jnp.concatenate([q_lat, q_rope], axis=-1).astype(jnp.bfloat16)
    col_scale = jnp.where(jnp.arange(WIDTH) < LATENT, lat_scale, 1.0)
    kv_cache = (jax.random.normal(key_cache, (BATCH, ROUNDS, GROUP, PAGE, WIDTH), jnp.float32) * col_scale).astype(jnp.bfloat16)
    lengths = jax.random.randint(key_len, (BATCH,), SEQ // 2, SEQ + 1, dtype=jnp.int32)
    longest = jax.random.randint(key_pick, (), 0, BATCH, dtype=jnp.int32)
    lengths = jnp.where(jnp.arange(BATCH) == longest, SEQ, lengths).astype(jnp.int32)
    return {'q_abs': q_abs, 'kv_cache': kv_cache, 'lengths': lengths}


def reference(q_abs, kv_cache, lengths):
    keys_all = kv_cache.reshape(BATCH, SEQ, WIDTH)
    score_scale = (NOPE + ROPE) ** -0.5
    positions = jnp.arange(SEQ)
    offsets = jnp.arange(MTP) - MTP

    def one_seq(seq_args):
        q_seq, key_seq, length = seq_args
        key_f = key_seq.astype(jnp.float32)
        scores = jnp.einsum('thd,sd->ths', q_seq.astype(jnp.float32), key_f) * score_scale
        last_pos = length + offsets
        visible = positions[None, :] <= last_pos[:, None]
        scores = jnp.where(visible[:, None, :], scores, -jnp.inf)
        weights = jax.nn.softmax(scores, axis=-1)
        out_seq = jnp.einsum('ths,sc->thc', weights, key_f[:, :LATENT])
        return out_seq.astype(jnp.bfloat16)

    return lax.map(one_seq, (q_abs, keys_all, lengths))
```

```python
import jax
import jax.numpy as jnp
from jax import lax
from jax.experimental import pallas as pl
from jax.experimental.pallas import tpu as pltpu
from jax.sharding import PartitionSpec as P

LATENT = 512
ROPE = 64
NOPE = 128
WIDTH = LATENT + ROPE
PAGE = 64
GROUP = 128
BATCH = 64
MASKED = -1e30
SCALE = (NOPE + ROPE) ** -0.5
MESH = pl.DeviceIdType.MESH

SZ, SY, SX = 32, 8, 2
RING = (SZ, SY, SX)
AX1 = (SY, SZ, SZ)
AX2 = (SX, SX, SY)
COUNT = (3, 3, 2)
BASE = (0, 24, 48)
SLOTS = 8


def pick(k, vals):
    return jnp.where(k == 0, vals[0], jnp.where(k == 1, vals[1], vals[2]))


def coord(me, stride):
    return lax.rem(lax.div(me, stride), 4)


def shifted(me, stride, d):
    c = coord(me, stride)
    return me + (lax.rem(c + d, 4) - c) * stride


def remote(src, dst, ssem, rsem, dev):
    return pltpu.make_async_remote_copy(src_ref=src, dst_ref=dst, send_sem=ssem, recv_sem=rsem, device_id={'dcp': dev}, device_id_type=MESH)


def kernel(len_ref, q_ref, kv_ref, out_ref, kvbuf, q0buf, qbuf, obuf, rsbuf, lbuf, lrecv, fsend, frecv,
           kv_s, kv_r, kv_l, q0_s, q0_r, q1_s, q1_r, q2_s, q2_r, rs_s, rs_r, l_s, l_r, f_s, f_r):
    me = lax.axis_index('dcp')
    core = lax.rem(me, 2)
    cx, cy, cz = coord(me, SX), coord(me, SY), coord(me, SZ)
    del cx, cy, cz

    bar = pltpu.get_barrier_semaphore()
    peers = [me + 1 - 2 * core]
    for s in (SZ, SY, SX):
        for d in (1, 2, 3):
            t = shifted(me, s, d)
            peers += [t, t + 1 - 2 * core]
    for s1, s2 in ((SZ, SY), (SZ, SX), (SY, SX)):
        for d1 in (1, 2, 3):
            for d2 in (1, 2, 3):
                peers.append(shifted(shifted(me, s1, d1), s2, d2))
    for t in peers:
        pl.semaphore_signal(bar, inc=1, device_id={'dcp': t}, device_id_type=MESH)
    lbuf[...] = jnp.zeros_like(lbuf)
    pl.semaphore_wait(bar, len(peers))

    own = [coord(me, RING[k]) * 2 + core for k in range(3)]

    def ring_dest(k, d, flip):
        dev = shifted(me, RING[k], d)
        dcore = core
        if flip:
            dev = dev + 1 - 2 * core
            dcore = 1 - core
        return dev, coord(dev, RING[k]) * 2 + dcore

    others = [(1, 0), (3, 0), (2, 0), (1, 1), (3, 1), (2, 1), (0, 1)]

    for k in range(3):
        for d, flip in others:
            dev, o = ring_dest(k, d, flip)
            remote(q_ref.at[k, o], q0buf.at[k, own[k]], q0_s.at[k], q0_r.at[k], dev).start()
        q0buf[k, own[k]] = q_ref[k, own[k]]

    def send_cache(t):
        k, i = t % 3, t // 3
        pltpu.make_async_copy(kv_ref.at[BASE[k] + own[k] * COUNT[k] + i, :, 0], kvbuf.at[t, own[k]], kv_l.at[t]).start()
        for d, flip in others:
            dev, o = ring_dest(k, d, flip)
            remote(kv_ref.at[BASE[k] + o * COUNT[k] + i, :, 0], kvbuf.at[t, own[k]], kv_s.at[t], kv_r.at[t], dev).start()

    for t in range(0, 3):
        send_cache(t)

    place = [coord(me, AX2[k]) * 4 + coord(me, AX1[k]) for k in range(3)]
    for k in range(3):
        n = COUNT[k]
        remote(q_ref.at[k, pl.ds(0, 7)], q0buf.at[k, pl.ds(0, 7)], q0_s.at[k], q0_r.at[k], me).wait_recv()
        row = lax.broadcasted_iota(jnp.int32, (n * 16, 128), 0)
        col = lax.broadcasted_iota(jnp.int32, (n * 16, 128), 1)
        want = (((row & 15) >> 1) << 4) + ((row >> 4) << 1) + (row & 1)
        perm = jnp.where(col == want, 1.0, 0.0).astype(jnp.bfloat16)
        rows = q0buf[k].reshape(128, WIDTH)
        piece = jnp.dot(perm, rows, preferred_element_type=jnp.float32).astype(jnp.bfloat16)
        qbuf[k, pl.ds(0, n), place[k]] = piece.reshape(n, 16, WIDTH)
        for d in (1, 3, 2):
            view = qbuf.at[k, pl.ds(0, n), place[k]]
            remote(view, view, q1_s.at[k], q1_r.at[k], shifted(me, AX1[k], d)).start()

    for t in range(3, 6):
        send_cache(t)

    for k in range(3):
        n = COUNT[k]
        three = qbuf.at[k, pl.ds(0, n), pl.ds(0, 3)]
        remote(three, three, q1_s.at[k], q1_r.at[k], me).wait_recv()
        view = qbuf.at[k, pl.ds(0, n), pl.ds(coord(me, AX2[k]) * 4, 4)]
        for d in (1, 3, 2):
            remote(view, view, q2_s.at[k], q2_r.at[k], shifted(me, AX2[k], d)).start()

    for t in range(6, SLOTS):
        send_cache(t)

    for k in range(3):
        n = COUNT[k]
        twelve = qbuf.at[k, pl.ds(0, n), pl.ds(0, 12)]
        remote(twelve, twelve, q2_s.at[k], q2_r.at[k], me).wait_recv()

    def attend(t, carry):
        k = lax.rem(t, 3)
        i = lax.div(t, 3)
        ring = pick(k, RING)
        u = coord(me, ring)
        o_me = u * 2 + core
        c1 = coord(me, pick(k, AX1))
        c2 = coord(me, pick(k, AX2))
        p_me = c2 * 4 + c1
        seq = 24 * k + o_me * pick(k, COUNT) + i
        length = len_ref[seq]
        pltpu.make_async_copy(kv_ref.at[0, :, 0], kvbuf.at[t, 0], kv_l.at[t]).wait()
        remote(kv_ref.at[pl.ds(0, 7), :, 0], kvbuf.at[t, pl.ds(0, 7)], kv_s.at[t], kv_r.at[t], me).wait_recv()
        q = qbuf[k, i].reshape(256, WIDTH)
        keys = kvbuf[t].reshape(1024, WIDTH)
        nt = (((1,), (1,)), ((), ()))
        s = lax.dot_general(q[:, :LATENT], keys[:, :LATENT], nt, preferred_element_type=jnp.float32)
        s = s + lax.dot_general(q[:, LATENT:], keys[:, LATENT:], nt, preferred_element_type=jnp.float32)
        s = s * SCALE
        kk = lax.broadcasted_iota(jnp.int32, (1, 1024), 1)
        dsrc = (me - u * ring - core) + (kk >> 8) * ring + ((kk >> 7) & 1)
        pos = (((kk >> 6) & 1) * GROUP + dsrc) * PAGE + (kk & 63)
        tok = lax.broadcasted_iota(jnp.int32, (256, 1), 0) & 1
        s = jnp.where(pos - tok <= length - 2, s, MASKED)
        m = jnp.max(s, axis=1, keepdims=True)
        w = jnp.exp(s - m)
        l = jnp.sum(w, axis=1, keepdims=True)
        part = jnp.dot(w.astype(jnp.bfloat16), keys[:, :LATENT], preferred_element_type=jnp.float32)
        part = (part * (1.0 / l)).astype(jnp.bfloat16)
        obuf[k, i] = part.reshape(16, 16, LATENT)
        lse = m + jnp.log(l)
        hi = lse.astype(jnp.bfloat16).astype(jnp.float32)
        mid = (lse - hi).astype(jnp.bfloat16).astype(jnp.float32)
        lo = lse - hi - mid
        lane = lax.broadcasted_iota(jnp.int32, (256, 128), 1)
        old = lbuf[k].reshape(256, 128).astype(jnp.float32)
        new = jnp.where(lane == i, hi, jnp.where(lane == 8 + i, mid, jnp.where(lane == 16 + i, lo, old)))
        lbuf[k] = new.astype(jnp.bfloat16).reshape(16, 16, 128)

        def dest(d1, d2):
            e1, e2 = lax.rem(c1 + d1, 4), lax.rem(c2 + d2, 4)
            return me + (e1 - c1) * pick(k, AX1) + (e2 - c2) * pick(k, AX2), e2 * 4 + e1

        order = [(d1, d2) for d1 in range(4) for d2 in range(4) if d1 or d2]
        for d1, d2 in order:
            dev, p = dest(d1, d2)
            remote(obuf.at[k, i, p], rsbuf.at[k, i, p_me], rs_s.at[t], rs_r.at[t], dev).start()
        rsbuf[k, i, p_me] = obuf[k, i, p_me]

        @pl.when(t >= 5)
        def _():
            for d1, d2 in order:
                dev, p = dest(d1, d2)
                remote(lbuf.at[k, p], lrecv.at[k, p_me], l_s.at[k], l_r.at[k], dev).start()
            lrecv[k, p_me] = lbuf[k, p_me]

        return carry

    lax.fori_loop(0, SLOTS, attend, 0)

    for k in (2, 0, 1):
        n = COUNT[k]
        remote(lbuf.at[k, pl.ds(0, 15)], lrecv.at[k, pl.ds(0, 15)], l_s.at[k], l_r.at[k], me).wait_recv()
        lr = lrecv[k].astype(jnp.float32)
        merged = []
        for i in range(n):
            t = 3 * i + k
            remote(obuf.at[k, i, pl.ds(0, 15)], rsbuf.at[k, i, pl.ds(0, 15)], rs_s.at[t], rs_r.at[t], me).wait_recv()
            lse = lr[:, :, i:i + 1] + lr[:, :, 8 + i:9 + i] + lr[:, :, 16 + i:17 + i]
            top = jnp.max(lse, axis=0, keepdims=True)
            e = jnp.exp(lse - top)
            wgt = e / jnp.sum(e, axis=0, keepdims=True)
            acc = wgt[0] * rsbuf[k, i, 0].astype(jnp.float32)
            for p in range(1, 16):
                acc = acc + wgt[p] * rsbuf[k, i, p].astype(jnp.float32)
            merged.append(acc.astype(jnp.bfloat16))
        rows = jnp.concatenate(merged, axis=0)
        row = lax.broadcasted_iota(jnp.int32, (128, n * 16), 0)
        col = lax.broadcasted_iota(jnp.int32, (128, n * 16), 1)
        have = (((col & 15) >> 1) << 4) + ((col >> 4) << 1) + (col & 1)
        perm = jnp.where(row == have, 1.0, 0.0).astype(jnp.bfloat16)
        fsend[k] = jnp.dot(perm, rows, preferred_element_type=jnp.float32).astype(jnp.bfloat16).reshape(8, 16, LATENT)
        for d, flip in others:
            dev, o = ring_dest(k, d, flip)
            remote(fsend.at[k, o], frecv.at[k, own[k]], f_s.at[k], f_r.at[k], dev).start()
        frecv[k, own[k]] = fsend[k, own[k]]

    for k in (2, 0, 1):
        remote(fsend.at[k, pl.ds(0, 7)], frecv.at[k, pl.ds(0, 7)], f_s.at[k], f_r.at[k], me).wait_recv()
        out_ref[k] = frecv[k]

    for t in range(SLOTS):
        k, i = t % 3, t // 3
        remote(kv_ref.at[pl.ds(0, 7), :, 0], kvbuf.at[t, pl.ds(0, 7)], kv_s.at[t], kv_r.at[t], me).wait_send()
        remote(obuf.at[k, i, pl.ds(0, 15)], rsbuf.at[k, i, pl.ds(0, 15)], rs_s.at[t], rs_r.at[t], me).wait_send()
    for k in range(3):
        n = COUNT[k]
        remote(q_ref.at[k, pl.ds(0, 7)], q0buf.at[k, pl.ds(0, 7)], q0_s.at[k], q0_r.at[k], me).wait_send()
        three = qbuf.at[k, pl.ds(0, n), pl.ds(0, 3)]
        remote(three, three, q1_s.at[k], q1_r.at[k], me).wait_send()
        twelve = qbuf.at[k, pl.ds(0, n), pl.ds(0, 12)]
        remote(twelve, twelve, q2_s.at[k], q2_r.at[k], me).wait_send()
        remote(lbuf.at[k, pl.ds(0, 15)], lrecv.at[k, pl.ds(0, 15)], l_s.at[k], l_r.at[k], me).wait_send()
        remote(fsend.at[k, pl.ds(0, 7)], frecv.at[k, pl.ds(0, 7)], f_s.at[k], f_r.at[k], me).wait_send()


def solution(mesh):
    bf16 = jnp.bfloat16

    def local_step(q_blk, kv_blk, len_blk):
        q = q_blk.reshape(BATCH * 2, WIDTH)
        sets = []
        for k in range(3):
            n = COUNT[k]
            block = q[2 * BASE[k]:2 * BASE[k] + 16 * n].reshape(8, 2 * n, WIDTH)
            sets.append(jnp.pad(block, ((0, 0), (0, 16 - 2 * n), (0, 0))))
        q_sets = jnp.stack(sets)
        dma = pltpu.SemaphoreType.DMA
        out = pl.pallas_call(
            kernel,
            out_shape=jax.ShapeDtypeStruct((3, 8, 16, LATENT), bf16),
            in_specs=[
                pl.BlockSpec(memory_space=pltpu.SMEM),
                pl.BlockSpec(memory_space=pltpu.VMEM),
                pl.BlockSpec(memory_space=pl.ANY),
            ],
            out_specs=pl.BlockSpec(memory_space=pltpu.VMEM),
            scratch_shapes=[
                pltpu.VMEM((SLOTS, 8, 2, PAGE, WIDTH), bf16),
                pltpu.VMEM((3, 8, 16, WIDTH), bf16),
                pltpu.VMEM((3, 3, 16, 16, WIDTH), bf16),
                pltpu.VMEM((3, 3, 16, 16, LATENT), bf16),
                pltpu.VMEM((3, 3, 16, 16, LATENT), bf16),
                pltpu.VMEM((3, 16, 16, 128), bf16),
                pltpu.VMEM((3, 16, 16, 128), bf16),
                pltpu.VMEM((3, 8, 16, LATENT), bf16),
                pltpu.VMEM((3, 8, 16, LATENT), bf16),
                dma((SLOTS,)), dma((SLOTS,)), dma((SLOTS,)),
                dma((3,)), dma((3,)),
                dma((3,)), dma((3,)),
                dma((3,)), dma((3,)),
                dma((SLOTS,)), dma((SLOTS,)),
                dma((3,)), dma((3,)),
                dma((3,)), dma((3,)),
            ],
            compiler_params=pltpu.CompilerParams(collective_id=0, has_side_effects=True, vmem_limit_bytes=56 * 1024 * 1024),
            name='mla',
        )(len_blk, q_sets, kv_blk)
        parts = [out[k, :, :2 * COUNT[k]].reshape(8 * COUNT[k], 2, 1, LATENT) for k in range(3)]
        return jnp.concatenate(parts, axis=0)

    return jax.shard_map(local_step, mesh=mesh, in_specs=(P('dp', None, 'dcp', None), P('dp', None, 'dcp', None, None), P('dp')), out_specs=P('dp', None, 'dcp', None), check_vma=False)
```

```python
import jax
import jax.numpy as jnp
from jax import lax
from jax.experimental import pallas as pl
from jax.experimental.pallas import tpu as pltpu
from jax.sharding import PartitionSpec as P

LATENT = 512
ROPE = 64
NOPE = 128
WIDTH = LATENT + ROPE
QW = LATENT + 2 * ROPE
PAGE = 64
GROUP = 128
BATCH = 64
MASKED = -1e30
SCALE = (NOPE + ROPE) ** -0.5
MESH = pl.DeviceIdType.MESH
BF16 = jnp.bfloat16
F32 = jnp.float32

SZ, SY, SX = 32, 8, 2
RING = (SZ, SY, SX)
BIG = (SX, SZ, SY)
SMALL = (SY, SX, SZ)
LAST_BIG = (True, False, True)
COUNT = (3, 3, 2)
BASE = (0, 24, 48)
SLOTS = 8


def pick(k, vals):
    return jnp.where(k == 0, vals[0], jnp.where(k == 1, vals[1], vals[2]))


def coord(me, stride):
    return lax.rem(lax.div(me, stride), 4)


def shifted(me, stride, d):
    c = coord(me, stride)
    return me + (lax.rem(c + d, 4) - c) * stride


def remote(src, dst, ssem, rsem, dev):
    return pltpu.make_async_remote_copy(src_ref=src, dst_ref=dst, send_sem=ssem, recv_sem=rsem, device_id={'dcp': dev}, device_id_type=MESH)


def split3(v):
    hi = v.astype(BF16).astype(F32)
    mid = (v - hi).astype(BF16).astype(F32)
    return hi, mid, v - hi - mid


def put_lse(old, lse, i):
    lane = lax.broadcasted_iota(jnp.int32, old.shape, len(old.shape) - 1)
    hi, mid, lo = split3(lse)
    return jnp.where(lane == i, hi, jnp.where(lane == 8 + i, mid, jnp.where(lane == 16 + i, lo, old)))


def get_lse(x, i):
    return x[..., i:i + 1] + x[..., 8 + i:9 + i] + x[..., 16 + i:17 + i]


def onehot(shape, fn):
    row = lax.broadcasted_iota(jnp.int32, shape, 0)
    col = lax.broadcasted_iota(jnp.int32, shape, 1)
    return jnp.where(fn(row, col), 1.0, 0.0).astype(BF16)


def by_set(rows, cols):
    mats = []
    for k in range(3):
        n = COUNT[k]
        mats.append(lambda r, c, k=k, n=n: (r < (k + 1) * 64) & (r >= k * 64) & ((r & 7) < 2 * n)
                    & (c == 2 * BASE[k] + ((r - k * 64) >> 3) * 2 * n + (r & 7)))
    return mats[0](rows, cols) | mats[1](rows, cols) | mats[2](rows, cols)


def kernel(len_ref, q_ref, kv_ref, out_ref, kvlocal, ropes, kvbuf, kvrope, qsend, q0buf, qbuf, obuf, r1buf, m1buf, r2buf,
           l1send, l1recv, l2send, l2recv, fsend, frecv,
           loc_s, kv_s, kv_r, kv_l, kr_s, kr_r, q0_s, q0_r, q1_s, q1_r, q2_s, q2_r, q3_s, q3_r, r1_s, r1_r, r2_s, r2_r,
           l1_s, l1_r, l2_s, l2_r, f_s, f_r):
    me = lax.axis_index('dcp')
    core = lax.rem(me, 2)
    local = pltpu.make_async_copy(kv_ref.at[:, :, 0], kvlocal, loc_s)
    local.start()

    bar = pltpu.get_barrier_semaphore()
    peers = [me + 1 - 2 * core]
    for s in (SZ, SY, SX):
        for d in (1, 2, 3):
            t = shifted(me, s, d)
            peers += [t, t + 1 - 2 * core]
    for t in peers:
        pl.semaphore_signal(bar, inc=1, device_id={'dcp': t}, device_id_type=MESH)

    perm = onehot((192, 128), by_set)
    rows = jnp.dot(perm, q_ref[...], preferred_element_type=F32).astype(BF16)
    qsend[:, :, :, pl.ds(0, LATENT)] = rows[:, :LATENT].reshape(3, 8, 8, LATENT)
    rope2 = jnp.concatenate([rows[:, LATENT:], rows[:, LATENT:]], axis=1)
    qsend[:, :, :, pl.ds(LATENT, 2 * ROPE)] = rope2.reshape(3, 8, 8, 2 * ROPE)
    l1send[...] = jnp.zeros_like(l1send)
    l2send[...] = jnp.zeros_like(l2send)
    pl.semaphore_wait(bar, len(peers))

    own = [coord(me, RING[k]) * 2 + core for k in range(3)]

    def ring_dest(k, d, flip):
        dev = shifted(me, RING[k], d)
        dcore = core
        if flip:
            dev = dev + 1 - 2 * core
            dcore = 1 - core
        return dev, coord(dev, RING[k]) * 2 + dcore

    others = [(1, 0), (3, 0), (2, 0), (1, 1), (3, 1), (2, 1), (0, 1)]

    for k in range(3):
        for d, flip in others:
            dev, o = ring_dest(k, d, flip)
            remote(qsend.at[k, o], q0buf.at[k, own[k]], q0_s.at[k], q0_r.at[k], dev).start()
        q0buf[k, own[k]] = qsend[k, own[k]]

    def latent(b):
        return kv_ref.at[b, :, 0, :, pl.ds(0, LATENT)]

    def send_cache(t, which):
        k, i = t % 3, t // 3
        for d, flip in which:
            dev, o = ring_dest(k, d, flip)
            remote(latent(BASE[k] + o * COUNT[k] + i), kvbuf.at[t, own[k]], kv_s.at[t], kv_r.at[t], dev).start()

    for t in range(3):
        send_cache(t, [(1, 0), (3, 0)])

    big = [coord(me, BIG[k]) for k in range(3)]
    small = [coord(me, SMALL[k]) for k in range(3)]
    for k in range(3):
        n = COUNT[k]
        remote(qsend.at[k, pl.ds(0, 7)], q0buf.at[k, pl.ds(0, 7)], q0_s.at[k], q0_r.at[k], me).wait_recv()
        order = onehot((n * 16, 64), lambda r, c: c == (((r & 15) >> 1) << 3) + ((r >> 4) << 1) + (r & 1))
        piece = jnp.dot(order, q0buf[k].reshape(64, QW), preferred_element_type=F32).astype(BF16)
        qbuf[k, pl.ds(0, n), big[k], small[k]] = piece.reshape(n, 16, QW)
        view = qbuf.at[k, pl.ds(0, n), big[k], small[k]]
        for d in (1, 3, 2):
            dev = shifted(me, SMALL[k] if LAST_BIG[k] else BIG[k], d)
            remote(view, view, q1_s.at[k], q1_r.at[k], dev).start()

    for t in range(3):
        send_cache(t, [(1, 1), (3, 1)])

    def block(k, idx, lo, cnt):
        n = COUNT[k]
        if LAST_BIG[k]:
            return qbuf.at[k, pl.ds(0, n), idx, pl.ds(lo, cnt)]
        return qbuf.at[k, pl.ds(0, n), pl.ds(lo, cnt), idx]

    mid = [big[k] if LAST_BIG[k] else small[k] for k in range(3)]
    axis = [BIG[k] if LAST_BIG[k] else SMALL[k] for k in range(3)]
    for k in range(3):
        three = block(k, 0, 0, 3)
        remote(three, three, q1_s.at[k], q1_r.at[k], me).wait_recv()
        view = block(k, mid[k], 0, 4)
        for j, d in enumerate((1, 3)):
            remote(view, view, q2_s.at[k, j], q2_r.at[k, j], shifted(me, axis[k], d)).start()

    local.wait()

    def pack(b, carry):
        ropes[b] = jnp.concatenate([kvlocal[b, 0, :, pl.ds(LATENT, ROPE)], kvlocal[b, 1, :, pl.ds(LATENT, ROPE)]], axis=1)
        return carry

    lax.fori_loop(0, BATCH, pack, 0, unroll=4)
    for k in range(3):
        n = COUNT[k]
        for d, flip in others:
            dev, o = ring_dest(k, d, flip)
            remote(ropes.at[pl.ds(BASE[k] + o * n, n)], kvrope.at[k, own[k], pl.ds(0, n)], kr_s.at[k], kr_r.at[k], dev).start()
        kvrope[k, own[k], pl.ds(0, n)] = ropes[pl.ds(BASE[k] + own[k] * n, n)]

    for t in range(3):
        send_cache(t, [(2, 0), (2, 1), (0, 1)])
    for t in range(SLOTS):
        k, i = t % 3, t // 3
        pltpu.make_async_copy(latent(BASE[k] + own[k] * COUNT[k] + i), kvbuf.at[t, own[k]], kv_l.at[t]).start()

    for k in range(3):
        for j, d in enumerate((1, 3)):
            whole = block(k, mid[k], 0, 4)
            remote(whole, whole, q2_s.at[k, j], q2_r.at[k, j], me).wait_recv()
            half = block(k, lax.rem(mid[k] + (3 if j == 0 else 1), 4), 2 * j, 2)
            remote(half, half, q3_s.at[k, j], q3_r.at[k, j], shifted(me, axis[k], d)).start()

    for t in range(3, SLOTS):
        send_cache(t, others)

    for k in range(3):
        n = COUNT[k]
        for j in range(2):
            half = block(k, mid[k], 0, 2)
            remote(half, half, q3_s.at[k, j], q3_r.at[k, j], me).wait_recv()
        seven = kvrope.at[k, pl.ds(0, 7), pl.ds(0, n)]
        remote(seven, seven, kr_s.at[k], kr_r.at[k], me).wait_recv()

    def attend(t, carry):
        k = lax.rem(t, 3)
        i = lax.div(t, 3)
        ring = pick(k, RING)
        u = coord(me, ring)
        bstride = pick(k, BIG)
        b_me = coord(me, bstride)
        length = len_ref[24 * k + (u * 2 + core) * pick(k, COUNT) + i]
        pltpu.make_async_copy(latent(0), kvbuf.at[t, 0], kv_l.at[t]).wait()
        seven = kvbuf.at[t, pl.ds(0, 7)]
        remote(seven, seven, kv_s.at[t], kv_r.at[t], me).wait_recv()
        q = qbuf[k, i].reshape(256, QW)
        keys = kvbuf[t].reshape(1024, LATENT)
        packed = kvrope[k, :, i]
        lane = lax.broadcasted_iota(jnp.int32, packed.shape, 2)
        zero = jnp.zeros_like(packed)
        rope = jnp.stack([jnp.where(lane < ROPE, packed, zero), jnp.where(lane >= ROPE, packed, zero)], axis=1).reshape(1024, 2 * ROPE)
        nt = (((1,), (1,)), ((), ()))
        s = lax.dot_general(q[:, :LATENT], keys, nt, preferred_element_type=F32)
        s = s + lax.dot_general(q[:, LATENT:], rope, nt, preferred_element_type=F32)
        s = s * SCALE
        kk = lax.broadcasted_iota(jnp.int32, (1, 1024), 1)
        dsrc = (me - u * ring - core) + (kk >> 8) * ring + ((kk >> 7) & 1)
        pos = (((kk >> 6) & 1) * GROUP + dsrc) * PAGE + (kk & 63)
        tok = lax.broadcasted_iota(jnp.int32, (256, 1), 0) & 1
        s = jnp.where(pos - tok <= length - 2, s, MASKED)
        m = jnp.max(s, axis=1, keepdims=True)
        w = jnp.exp(s - m)
        l = jnp.sum(w, axis=1, keepdims=True)
        part = jnp.dot(w.astype(BF16), keys, preferred_element_type=F32)
        obuf[k, i] = (part * (1.0 / l)).astype(BF16).reshape(4, 4, 16, LATENT)
        old = l1send[k].reshape(256, 128).astype(F32)
        l1send[k] = put_lse(old, m + jnp.log(l), i).astype(BF16).reshape(4, 4, 16, 128)
        for d in (1, 3, 2):
            b = lax.rem(b_me + d, 4)
            remote(obuf.at[k, i, b], r1buf.at[k, i, b_me], r1_s.at[t], r1_r.at[t], me + (b - b_me) * bstride).start()
        r1buf[k, i, b_me] = obuf[k, i, b_me]

        @pl.when(t >= 5)
        def _():
            for d in (1, 3, 2):
                b = lax.rem(b_me + d, 4)
                remote(l1send.at[k, b], l1recv.at[k, b_me], l1_s.at[k], l1_r.at[k], me + (b - b_me) * bstride).start()
            l1recv[k, b_me] = l1send[k, b_me]

        return carry

    lax.fori_loop(0, SLOTS, attend, 0)

    def merge(lse, ref):
        top = jnp.max(lse, axis=0)
        e = jnp.exp(lse - top[None])
        total = jnp.sum(e, axis=0)
        wgt = e / total[None]
        acc = wgt[0] * ref[0].astype(F32)
        for p in range(1, 4):
            acc = acc + wgt[p] * ref[p].astype(F32)
        return acc.astype(BF16), top + jnp.log(total)

    for k in (2, 0, 1):
        n = COUNT[k]
        three = l1recv.at[k, pl.ds(0, 3)]
        remote(three, three, l1_s.at[k], l1_r.at[k], me).wait_recv()
        lr = l1recv[k].astype(F32)
        lacc = jnp.zeros((4, 16, 128), F32)
        for i in range(n):
            t = 3 * i + k
            three = r1buf.at[k, i, pl.ds(0, 3)]
            remote(three, three, r1_s.at[t], r1_r.at[t], me).wait_recv()
            both, lse = merge(get_lse(lr, i), r1buf.at[k, i])
            m1buf[k, i] = both
            lacc = put_lse(lacc, lse, i)
            for d in (1, 3, 2):
                b = lax.rem(small[k] + d, 4)
                remote(m1buf.at[k, i, b], r2buf.at[k, i, small[k]], r2_s.at[t], r2_r.at[t], shifted(me, SMALL[k], d)).start()
            r2buf[k, i, small[k]] = m1buf[k, i, small[k]]
        l2send[k] = lacc.astype(BF16)
        for d in (1, 3, 2):
            b = lax.rem(small[k] + d, 4)
            remote(l2send.at[k, b], l2recv.at[k, small[k]], l2_s.at[k], l2_r.at[k], shifted(me, SMALL[k], d)).start()
        l2recv[k, small[k]] = l2send[k, small[k]]

    for k in (2, 0, 1):
        n = COUNT[k]
        three = l2recv.at[k, pl.ds(0, 3)]
        remote(three, three, l2_s.at[k], l2_r.at[k], me).wait_recv()
        lr = l2recv[k].astype(F32)
        merged = []
        for i in range(n):
            t = 3 * i + k
            three = r2buf.at[k, i, pl.ds(0, 3)]
            remote(three, three, r2_s.at[t], r2_r.at[t], me).wait_recv()
            merged.append(merge(get_lse(lr, i), r2buf.at[k, i])[0])
        order = onehot((64, n * 16), lambda r, c: r == (((c & 15) >> 1) << 3) + ((c >> 4) << 1) + (c & 1))
        out = jnp.dot(order, jnp.concatenate(merged, axis=0), preferred_element_type=F32)
        fsend[k] = out.astype(BF16).reshape(8, 8, LATENT)
        for d, flip in others:
            dev, o = ring_dest(k, d, flip)
            remote(fsend.at[k, o], frecv.at[k, own[k]], f_s.at[k], f_r.at[k], dev).start()
        frecv[k, own[k]] = fsend[k, own[k]]

    back = onehot((128, 192), lambda r, c: by_set(c, r))
    for k in range(3):
        seven = frecv.at[k, pl.ds(0, 7)]
        remote(seven, seven, f_s.at[k], f_r.at[k], me).wait_recv()
    out_ref[...] = jnp.dot(back, frecv[...].reshape(192, LATENT), preferred_element_type=F32).astype(BF16)

    def sent(view, sem):
        remote(view, view, sem, sem, me).wait_send()

    for t in range(SLOTS):
        k, i = t % 3, t // 3
        sent(kvbuf.at[t, pl.ds(0, 7)], kv_s.at[t])
        sent(r1buf.at[k, i, pl.ds(0, 3)], r1_s.at[t])
        sent(r2buf.at[k, i, pl.ds(0, 3)], r2_s.at[t])
    for k in range(3):
        n = COUNT[k]
        sent(q0buf.at[k, pl.ds(0, 7)], q0_s.at[k])
        sent(block(k, 0, 0, 3), q1_s.at[k])
        for j in range(2):
            sent(block(k, 0, 0, 4), q2_s.at[k, j])
            sent(block(k, 0, 0, 2), q3_s.at[k, j])
        sent(kvrope.at[k, pl.ds(0, 7), pl.ds(0, n)], kr_s.at[k])
        sent(l1recv.at[k, pl.ds(0, 3)], l1_s.at[k])
        sent(l2recv.at[k, pl.ds(0, 3)], l2_s.at[k])
        sent(frecv.at[k, pl.ds(0, 7)], f_s.at[k])


def solution(mesh):
    def local_step(q_blk, kv_blk, len_blk):
        dma = pltpu.SemaphoreType.DMA
        vmem = pltpu.VMEM
        out = pl.pallas_call(
            kernel,
            out_shape=jax.ShapeDtypeStruct((2 * BATCH, LATENT), BF16),
            in_specs=[
                pl.BlockSpec(memory_space=pltpu.SMEM),
                pl.BlockSpec(memory_space=pltpu.VMEM),
                pl.BlockSpec(memory_space=pl.ANY),
            ],
            out_specs=pl.BlockSpec(memory_space=pltpu.VMEM),
            scratch_shapes=[
                vmem((BATCH, 2, PAGE, WIDTH), BF16),
                vmem((BATCH, PAGE, 2 * ROPE), BF16),
                vmem((SLOTS, 8, 2, PAGE, LATENT), BF16),
                vmem((3, 8, 3, PAGE, 2 * ROPE), BF16),
                vmem((3, 8, 8, QW), BF16),
                vmem((3, 8, 8, QW), BF16),
                vmem((3, 3, 4, 4, 16, QW), BF16),
                vmem((3, 3, 4, 4, 16, LATENT), BF16),
                vmem((3, 3, 4, 4, 16, LATENT), BF16),
                vmem((3, 3, 4, 16, LATENT), BF16),
                vmem((3, 3, 4, 16, LATENT), BF16),
                vmem((3, 4, 4, 16, 128), BF16),
                vmem((3, 4, 4, 16, 128), BF16),
                vmem((3, 4, 16, 128), BF16),
                vmem((3, 4, 16, 128), BF16),
                vmem((3, 8, 8, LATENT), BF16),
                vmem((3, 8, 8, LATENT), BF16),
                dma,
                dma((SLOTS,)), dma((SLOTS,)), dma((SLOTS,)),
                dma((3,)), dma((3,)),
                dma((3,)), dma((3,)),
                dma((3,)), dma((3,)),
                dma((3, 2)), dma((3, 2)),
                dma((3, 2)), dma((3, 2)),
                dma((SLOTS,)), dma((SLOTS,)),
                dma((SLOTS,)), dma((SLOTS,)),
                dma((3,)), dma((3,)),
                dma((3,)), dma((3,)),
                dma((3,)), dma((3,)),
            ],
            compiler_params=pltpu.CompilerParams(collective_id=0, has_side_effects=True, vmem_limit_bytes=60 * 1024 * 1024),
            name='mla',
        )(len_blk, q_blk.reshape(2 * BATCH, WIDTH), kv_blk)
        return out.reshape(BATCH, 2, 1, LATENT)

    return jax.shard_map(local_step, mesh=mesh, in_specs=(P('dp', None, 'dcp', None), P('dp', None, 'dcp', None, None), P('dp')), out_specs=P('dp', None, 'dcp', None), check_vma=False)
```

```python
import jax
import jax.numpy as jnp
from jax import lax
from jax.experimental import pallas as pl
from jax.experimental.pallas import tpu as pltpu
from jax.sharding import PartitionSpec as P

LATENT = 512
ROPE = 64
NOPE = 128
WIDTH = LATENT + ROPE
QW = LATENT + 2 * ROPE
PAGE = 64
GROUP = 128
BATCH = 64
MASKED = -1e30
SCALE = (NOPE + ROPE) ** -0.5
MESH = pl.DeviceIdType.MESH
BF16 = jnp.bfloat16
F32 = jnp.float32

SZ, SY, SX = 32, 8, 2
RING = (SZ, SY, SX)
BIG = (SX, SZ, SY)
SMALL = (SY, SX, SZ)
LAST_BIG = (True, False, True)
COUNT = (3, 3, 2)
BASE = (0, 24, 48)
SLOTS = 8


def pick(k, vals):
    return jnp.where(k == 0, vals[0], jnp.where(k == 1, vals[1], vals[2]))


def coord(me, stride):
    return lax.rem(lax.div(me, stride), 4)


def shifted(me, stride, d):
    c = coord(me, stride)
    return me + (lax.rem(c + d, 4) - c) * stride


def remote(src, dst, ssem, rsem, dev):
    return pltpu.make_async_remote_copy(src_ref=src, dst_ref=dst, send_sem=ssem, recv_sem=rsem, device_id={'dcp': dev}, device_id_type=MESH)


def split3(v):
    hi = v.astype(BF16).astype(F32)
    mid = (v - hi).astype(BF16).astype(F32)
    return hi, mid, v - hi - mid


def put_lse(old, lse, i):
    lane = lax.broadcasted_iota(jnp.int32, old.shape, len(old.shape) - 1)
    hi, mid, lo = split3(lse)
    return jnp.where(lane == i, hi, jnp.where(lane == 8 + i, mid, jnp.where(lane == 16 + i, lo, old)))


def get_lse(x, i):
    return x[..., i:i + 1] + x[..., 8 + i:9 + i] + x[..., 16 + i:17 + i]


def onehot(shape, fn):
    row = lax.broadcasted_iota(jnp.int32, shape, 0)
    col = lax.broadcasted_iota(jnp.int32, shape, 1)
    return jnp.where(fn(row, col), 1.0, 0.0).astype(BF16)


def by_set(rows, cols):
    mats = []
    for k in range(3):
        n = COUNT[k]
        mats.append(lambda r, c, k=k, n=n: (r < (k + 1) * 64) & (r >= k * 64) & ((r & 7) < 2 * n)
                    & (c == 2 * BASE[k] + ((r - k * 64) >> 3) * 2 * n + (r & 7)))
    return mats[0](rows, cols) | mats[1](rows, cols) | mats[2](rows, cols)


def kernel(len_ref, q_ref, kv_ref, out_ref, qlocal, kvlocal, ropes, kvbuf, kvrope, qsend, q0buf, qbuf, obuf, r1buf, m1buf, r2buf,
           l1send, l1recv, l2send, l2recv, fsend, frecv,
           ql_s, loc_s, kv_s, kv_r, kv_l, kr_s, kr_r, q0_s, q0_r, q1_s, q1_r, q2_s, q2_r, q3_s, q3_r, r1_s, r1_r, r2_s, r2_r,
           l1_s, l1_r, l2_s, l2_r, f_s, f_r):
    me = lax.axis_index('dcp')
    core = lax.rem(me, 2)
    queries = pltpu.make_async_copy(q_ref, qlocal, ql_s)
    queries.start()
    local = pltpu.make_async_copy(kv_ref.at[:, :, 0], kvlocal, loc_s)
    local.start()

    bar = pltpu.get_barrier_semaphore()
    peers = [me + 1 - 2 * core]
    for s in (SZ, SY, SX):
        for d in (1, 2, 3):
            t = shifted(me, s, d)
            peers += [t, t + 1 - 2 * core]
    for t in peers:
        pl.semaphore_signal(bar, inc=1, device_id={'dcp': t}, device_id_type=MESH)
    perm = onehot((192, 128), by_set)
    queries.wait()
    rows = jnp.dot(perm, qlocal[...].reshape(2 * BATCH, WIDTH), preferred_element_type=F32).astype(BF16)
    qsend[:, :, :, pl.ds(0, LATENT)] = rows[:, :LATENT].reshape(3, 8, 8, LATENT)
    rope2 = jnp.concatenate([rows[:, LATENT:], rows[:, LATENT:]], axis=1)
    qsend[:, :, :, pl.ds(LATENT, 2 * ROPE)] = rope2.reshape(3, 8, 8, 2 * ROPE)
    l1send[...] = jnp.zeros_like(l1send)
    l2send[...] = jnp.zeros_like(l2send)
    pl.semaphore_wait(bar, len(peers))
    own = [coord(me, RING[k]) * 2 + core for k in range(3)]

    def ring_dest(k, d, flip):
        dev = shifted(me, RING[k], d)
        dcore = core
        if flip:
            dev = dev + 1 - 2 * core
            dcore = 1 - core
        return dev, coord(dev, RING[k]) * 2 + dcore

    others = [(1, 0), (3, 0), (2, 0), (1, 1), (3, 1), (2, 1), (0, 1)]

    for k in range(3):
        for d, flip in others:
            dev, o = ring_dest(k, d, flip)
            remote(qsend.at[k, o], q0buf.at[k, own[k]], q0_s.at[k], q0_r.at[k], dev).start()
        q0buf[k, own[k]] = qsend[k, own[k]]

    def latent(b):
        return kv_ref.at[b, :, 0, :, pl.ds(0, LATENT)]

    def send_cache(t, which):
        k, i = t % 3, t // 3
        for d, flip in which:
            dev, o = ring_dest(k, d, flip)
            remote(latent(BASE[k] + o * COUNT[k] + i), kvbuf.at[t, own[k]], kv_s.at[t], kv_r.at[t], dev).start()
    for t in range(3):
        send_cache(t, others[:2] + others[3:5])
    send_cache(2, [(2, 0), (2, 1), (0, 1)])
    big = [coord(me, BIG[k]) for k in range(3)]
    small = [coord(me, SMALL[k]) for k in range(3)]
    for k in range(3):
        n = COUNT[k]
        remote(qsend.at[k, pl.ds(0, 7)], q0buf.at[k, pl.ds(0, 7)], q0_s.at[k], q0_r.at[k], me).wait_recv()
        order = onehot((n * 16, 64), lambda r, c: c == (((r & 15) >> 1) << 3) + ((r >> 4) << 1) + (r & 1))
        piece = jnp.dot(order, q0buf[k].reshape(64, QW), preferred_element_type=F32).astype(BF16)
        qbuf[k, pl.ds(0, n), big[k], small[k]] = piece.reshape(n, 16, QW)
        view = qbuf.at[k, pl.ds(0, n), big[k], small[k]]
        for d in (1, 3, 2):
            dev = shifted(me, SMALL[k] if LAST_BIG[k] else BIG[k], d)
            remote(view, view, q1_s.at[k], q1_r.at[k], dev).start()
    for t in range(2):
        send_cache(t, [(2, 0), (2, 1), (0, 1)])

    def block(k, idx, lo, cnt):
        n = COUNT[k]
        if LAST_BIG[k]:
            return qbuf.at[k, pl.ds(0, n), idx, pl.ds(lo, cnt)]
        return qbuf.at[k, pl.ds(0, n), pl.ds(lo, cnt), idx]
    mid = [big[k] if LAST_BIG[k] else small[k] for k in range(3)]
    axis = [BIG[k] if LAST_BIG[k] else SMALL[k] for k in range(3)]
    for k in range(3):
        three = block(k, 0, 0, 3)
        remote(three, three, q1_s.at[k], q1_r.at[k], me).wait_recv()
        view = block(k, mid[k], 0, 4)
        for j, d in enumerate((1, 3)):
            remote(view, view, q2_s.at[k, j], q2_r.at[k, j], shifted(me, axis[k], d)).start()
    local.wait()
    def pack(b, carry):
        ropes[b] = jnp.concatenate([kvlocal[b, 0, :, pl.ds(LATENT, ROPE)], kvlocal[b, 1, :, pl.ds(LATENT, ROPE)]], axis=1)
        return carry

    lax.fori_loop(0, BATCH, pack, 0, unroll=4)
    for k in range(3):
        n = COUNT[k]
        for d, flip in others:
            dev, o = ring_dest(k, d, flip)
            remote(ropes.at[pl.ds(BASE[k] + o * n, n)], kvrope.at[k, own[k], pl.ds(0, n)], kr_s.at[k], kr_r.at[k], dev).start()
        kvrope[k, own[k], pl.ds(0, n)] = ropes[pl.ds(BASE[k] + own[k] * n, n)]

    send_cache(3, others)
    send_cache(4, others[:2])
    send_cache(5, others[:2])

    def forward(k):
        for j, d in enumerate((1, 3)):
            whole = block(k, mid[k], 0, 4)
            remote(whole, whole, q2_s.at[k, j], q2_r.at[k, j], me).wait_recv()
            half = block(k, lax.rem(mid[k] + (3 if j == 0 else 1), 4), 2 * j, 2)
            remote(half, half, q3_s.at[k, j], q3_r.at[k, j], shifted(me, axis[k], d)).start()
    forward(2)
    send_cache(4, others[2:])
    send_cache(6, others)
    send_cache(7, others)
    forward(0)
    forward(1)
    send_cache(5, others[2:])
    for t in range(SLOTS):
        k, i = t % 3, t // 3
        pltpu.make_async_copy(latent(BASE[k] + own[k] * COUNT[k] + i), kvbuf.at[t, own[k]], kv_l.at[t]).start()
    for k in range(3):
        n = COUNT[k]
        for j in range(2):
            half = block(k, mid[k], 0, 2)
            remote(half, half, q3_s.at[k, j], q3_r.at[k, j], me).wait_recv()
        seven = kvrope.at[k, pl.ds(0, 7), pl.ds(0, n)]
        remote(seven, seven, kr_s.at[k], kr_r.at[k], me).wait_recv()
    def attend(t, carry):
        k = lax.rem(t, 3)
        i = lax.div(t, 3)
        ring = pick(k, RING)
        u = coord(me, ring)
        bstride = pick(k, BIG)
        b_me = coord(me, bstride)
        length = len_ref[24 * k + (u * 2 + core) * pick(k, COUNT) + i]
        pltpu.make_async_copy(latent(0), kvbuf.at[t, 0], kv_l.at[t]).wait()
        seven = kvbuf.at[t, pl.ds(0, 7)]
        remote(seven, seven, kv_s.at[t], kv_r.at[t], me).wait_recv()
        q = qbuf[k, i].reshape(256, QW)
        keys = kvbuf[t].reshape(1024, LATENT)
        packed = kvrope[k, :, i]
        lane = lax.broadcasted_iota(jnp.int32, packed.shape, 2)
        zero = jnp.zeros_like(packed)
        rope = jnp.stack([jnp.where(lane < ROPE, packed, zero), jnp.where(lane >= ROPE, packed, zero)], axis=1).reshape(1024, 2 * ROPE)
        nt = (((1,), (1,)), ((), ()))
        s = lax.dot_general(q[:, :LATENT], keys, nt, preferred_element_type=F32)
        s = s + lax.dot_general(q[:, LATENT:], rope, nt, preferred_element_type=F32)
        s = s * SCALE
        kk = lax.broadcasted_iota(jnp.int32, (1, 1024), 1)
        dsrc = (me - u * ring - core) + (kk >> 8) * ring + ((kk >> 7) & 1)
        pos = (((kk >> 6) & 1) * GROUP + dsrc) * PAGE + (kk & 63)
        tok = lax.broadcasted_iota(jnp.int32, (256, 1), 0) & 1
        s = jnp.where(pos - tok <= length - 2, s, MASKED)
        m = jnp.max(s, axis=1, keepdims=True)
        w = jnp.exp(s - m)
        l = jnp.sum(w, axis=1, keepdims=True)
        part = jnp.dot(w.astype(BF16), keys, preferred_element_type=F32)
        obuf[k, i] = (part * (1.0 / l)).astype(BF16).reshape(4, 4, 16, LATENT)
        old = l1send[k].reshape(256, 128).astype(F32)
        l1send[k] = put_lse(old, m + jnp.log(l), i).astype(BF16).reshape(4, 4, 16, 128)
        for d in (1, 3, 2):
            b = lax.rem(b_me + d, 4)
            remote(obuf.at[k, i, b], r1buf.at[k, i, b_me], r1_s.at[t], r1_r.at[t], me + (b - b_me) * bstride).start()
        r1buf[k, i, b_me] = obuf[k, i, b_me]

        @pl.when(t >= 5)
        def _():
            for d in (1, 3, 2):
                b = lax.rem(b_me + d, 4)
                remote(l1send.at[k, b], l1recv.at[k, b_me], l1_s.at[k], l1_r.at[k], me + (b - b_me) * bstride).start()
            l1recv[k, b_me] = l1send[k, b_me]
        return carry

    lax.fori_loop(0, SLOTS, attend, 0)

    def merge(lse, ref):
        top = jnp.max(lse, axis=0)
        e = jnp.exp(lse - top[None])
        total = jnp.sum(e, axis=0)
        wgt = e / total[None]
        acc = wgt[0] * ref[0].astype(F32)
        for p in range(1, 4):
            acc = acc + wgt[p] * ref[p].astype(F32)
        return acc.astype(BF16), top + jnp.log(total)

    for k in (2, 0, 1):
        n = COUNT[k]
        three = l1recv.at[k, pl.ds(0, 3)]
        remote(three, three, l1_s.at[k], l1_r.at[k], me).wait_recv()
        lr = l1recv[k].astype(F32)
        lacc = jnp.zeros((4, 16, 128), F32)
        for i in range(n):
            t = 3 * i + k
            three = r1buf.at[k, i, pl.ds(0, 3)]
            remote(three, three, r1_s.at[t], r1_r.at[t], me).wait_recv()
            both, lse = merge(get_lse(lr, i), r1buf.at[k, i])
            m1buf[k, i] = both
            lacc = put_lse(lacc, lse, i)
            for d in (1, 3, 2):
                b = lax.rem(small[k] + d, 4)
                remote(m1buf.at[k, i, b], r2buf.at[k, i, small[k]], r2_s.at[t], r2_r.at[t], shifted(me, SMALL[k], d)).start()
            r2buf[k, i, small[k]] = m1buf[k, i, small[k]]
        l2send[k] = lacc.astype(BF16)
        for d in (1, 3, 2):
            b = lax.rem(small[k] + d, 4)
            remote(l2send.at[k, b], l2recv.at[k, small[k]], l2_s.at[k], l2_r.at[k], shifted(me, SMALL[k], d)).start()
        l2recv[k, small[k]] = l2send[k, small[k]]

    for k in (2, 0, 1):
        n = COUNT[k]
        three = l2recv.at[k, pl.ds(0, 3)]
        remote(three, three, l2_s.at[k], l2_r.at[k], me).wait_recv()
        lr = l2recv[k].astype(F32)
        merged = []
        for i in range(n):
            t = 3 * i + k
            three = r2buf.at[k, i, pl.ds(0, 3)]
            remote(three, three, r2_s.at[t], r2_r.at[t], me).wait_recv()
            merged.append(merge(get_lse(lr, i), r2buf.at[k, i])[0])
        order = onehot((64, n * 16), lambda r, c: r == (((c & 15) >> 1) << 3) + ((c >> 4) << 1) + (c & 1))
        out = jnp.dot(order, jnp.concatenate(merged, axis=0), preferred_element_type=F32)
        fsend[k] = out.astype(BF16).reshape(8, 8, LATENT)
        for d, flip in others:
            dev, o = ring_dest(k, d, flip)
            remote(fsend.at[k, o], frecv.at[k, own[k]], f_s.at[k], f_r.at[k], dev).start()
        frecv[k, own[k]] = fsend[k, own[k]]
    back = onehot((128, 192), lambda r, c: by_set(c, r))
    for k in range(3):
        seven = frecv.at[k, pl.ds(0, 7)]
        remote(seven, seven, f_s.at[k], f_r.at[k], me).wait_recv()
    out = jnp.dot(back, frecv[...].reshape(192, LATENT), preferred_element_type=F32)
    out_ref[...] = out.astype(BF16).reshape(BATCH, 2, LATENT)
    def sent(view, sem):
        remote(view, view, sem, sem, me).wait_send()

    for t in range(SLOTS):
        k, i = t % 3, t // 3
        sent(kvbuf.at[t, pl.ds(0, 7)], kv_s.at[t])
        sent(r1buf.at[k, i, pl.ds(0, 3)], r1_s.at[t])
        sent(r2buf.at[k, i, pl.ds(0, 3)], r2_s.at[t])
    for k in range(3):
        n = COUNT[k]
        sent(q0buf.at[k, pl.ds(0, 7)], q0_s.at[k])
        sent(block(k, 0, 0, 3), q1_s.at[k])
        for j in range(2):
            sent(block(k, 0, 0, 4), q2_s.at[k, j])
            sent(block(k, 0, 0, 2), q3_s.at[k, j])
        sent(kvrope.at[k, pl.ds(0, 7), pl.ds(0, n)], kr_s.at[k])
        sent(l1recv.at[k, pl.ds(0, 3)], l1_s.at[k])
        sent(l2recv.at[k, pl.ds(0, 3)], l2_s.at[k])
        sent(frecv.at[k, pl.ds(0, 7)], f_s.at[k])


def solution(mesh):
    def local_step(q_blk, kv_blk, len_blk):
        dma = pltpu.SemaphoreType.DMA
        vmem = pltpu.VMEM
        out = pl.pallas_call(
            kernel,
            out_shape=jax.ShapeDtypeStruct((BATCH, 2, LATENT), BF16),
            in_specs=[
                pl.BlockSpec(memory_space=pltpu.SMEM),
                pl.BlockSpec(memory_space=pltpu.HBM),
                pl.BlockSpec(memory_space=pltpu.HBM),
            ],
            out_specs=pl.BlockSpec(memory_space=pltpu.VMEM),
            scratch_shapes=[
                vmem((BATCH, 2, WIDTH), BF16),
                vmem((BATCH, 2, PAGE, WIDTH), BF16),
                vmem((BATCH, PAGE, 2 * ROPE), BF16),
                vmem((SLOTS, 8, 2, PAGE, LATENT), BF16),
                vmem((3, 8, 3, PAGE, 2 * ROPE), BF16),
                vmem((3, 8, 8, QW), BF16),
                vmem((3, 8, 8, QW), BF16),
                vmem((3, 3, 4, 4, 16, QW), BF16),
                vmem((3, 3, 4, 4, 16, LATENT), BF16),
                vmem((3, 3, 4, 4, 16, LATENT), BF16),
                vmem((3, 3, 4, 16, LATENT), BF16),
                vmem((3, 3, 4, 16, LATENT), BF16),
                vmem((3, 4, 4, 16, 128), BF16),
                vmem((3, 4, 4, 16, 128), BF16),
                vmem((3, 4, 16, 128), BF16),
                vmem((3, 4, 16, 128), BF16),
                vmem((3, 8, 8, LATENT), BF16),
                vmem((3, 8, 8, LATENT), BF16),
                dma, dma,
                dma((SLOTS,)), dma((SLOTS,)), dma((SLOTS,)),
                dma((3,)), dma((3,)),
                dma((3,)), dma((3,)),
                dma((3,)), dma((3,)),
                dma((3, 2)), dma((3, 2)),
                dma((3, 2)), dma((3, 2)),
                dma((SLOTS,)), dma((SLOTS,)),
                dma((SLOTS,)), dma((SLOTS,)),
                dma((3,)), dma((3,)),
                dma((3,)), dma((3,)),
                dma((3,)), dma((3,)),
            ],
            compiler_params=pltpu.CompilerParams(collective_id=0, has_side_effects=True, vmem_limit_bytes=44 * 1024 * 1024),
            name='mla',
        )(len_blk, q_blk.reshape(BATCH, 2, WIDTH), kv_blk)
        return out.reshape(BATCH, 2, 1, LATENT)

    return jax.shard_map(local_step, mesh=mesh, in_specs=(P('dp', None, 'dcp', None), P('dp', None, 'dcp', None, None), P('dp')), out_specs=P('dp', None, 'dcp', None), check_vma=False)
```

```python
import jax
import jax.numpy as jnp
from jax import lax
from jax.experimental import pallas as pl
from jax.experimental.pallas import tpu as pltpu
from jax.sharding import PartitionSpec as P

LATENT = 512
ROPE = 64
NOPE = 128
WIDTH = LATENT + ROPE
QW = LATENT + 2 * ROPE
PAGE = 64
GROUP = 128
BATCH = 64
MASKED = -1e30
SCALE = (NOPE + ROPE) ** -0.5
MESH = pl.DeviceIdType.MESH
BF16 = jnp.bfloat16
F32 = jnp.float32

SZ, SY, SX = 32, 8, 2
RING = (SZ, SY, SX)
BIG = (SX, SZ, SY)
SMALL = (SY, SX, SZ)
LAST_BIG = (True, False, True)
COUNT = (3, 3, 2)
BASE = (0, 24, 48)
SLOTS = 8


def pick(k, vals):
    return jnp.where(k == 0, vals[0], jnp.where(k == 1, vals[1], vals[2]))


def coord(me, stride):
    return lax.rem(lax.div(me, stride), 4)


def shifted(me, stride, d):
    c = coord(me, stride)
    return me + (lax.rem(c + d, 4) - c) * stride


def remote(src, dst, ssem, rsem, dev):
    return pltpu.make_async_remote_copy(src_ref=src, dst_ref=dst, send_sem=ssem, recv_sem=rsem, device_id={'dcp': dev}, device_id_type=MESH)


def split3(v):
    hi = v.astype(BF16).astype(F32)
    mid = (v - hi).astype(BF16).astype(F32)
    return hi, mid, v - hi - mid


def put_lse(old, lse, i):
    lane = lax.broadcasted_iota(jnp.int32, old.shape, len(old.shape) - 1)
    hi, mid, lo = split3(lse)
    return jnp.where(lane == i, hi, jnp.where(lane == 8 + i, mid, jnp.where(lane == 16 + i, lo, old)))


def tile_lse(lse):
    tile = jnp.zeros((4, 16, 128), F32)
    lane = lax.broadcasted_iota(jnp.int32, tile.shape, 2)
    for b in range(4):
        for j, v in enumerate(split3(lse[:, b])):
            tile = jnp.where(lane == 32 * b + j, v, tile)
    return tile.astype(BF16)


def untile_lse(x):
    return jnp.stack([x[..., 32 * b:32 * b + 1] + x[..., 32 * b + 1:32 * b + 2] + x[..., 32 * b + 2:32 * b + 3] for b in range(4)], axis=1)


def get_lse(x, i):
    return x[..., i:i + 1] + x[..., 8 + i:9 + i] + x[..., 16 + i:17 + i]


def onehot(shape, fn):
    row = lax.broadcasted_iota(jnp.int32, shape, 0)
    col = lax.broadcasted_iota(jnp.int32, shape, 1)
    return jnp.where(fn(row, col), 1.0, 0.0).astype(BF16)


def by_set(rows, cols):
    mats = []
    for k in range(3):
        n = COUNT[k]
        mats.append(lambda r, c, k=k, n=n: (r < (k + 1) * 64) & (r >= k * 64) & ((r & 7) < 2 * n)
                    & (c == 2 * BASE[k] + ((r - k * 64) >> 3) * 2 * n + (r & 7)))
    return mats[0](rows, cols) | mats[1](rows, cols) | mats[2](rows, cols)


def kernel(len_hbm, q_ref, kv_ref, out_ref, len_ref, qlocal, kvlocal, ropes, kvbuf, kvrope, qsend, q0buf, qbuf, obuf, r1buf, m1buf, r2buf,
           l1send, l1recv, l2send, l2recv, fsend, frecv,
           len_s, ql_s, loc_s, kv_s, kv_r, kv_l, kr_s, kr_r, q0_s, q0_r, q1_s, q1_r, q2_s, q2_r, q3_s, q3_r, r1_s, r1_r, r2_s, r2_r,
           l1_s, l1_r, l2_s, l2_r, f_s, f_r):
    me = lax.axis_index('dcp')
    core = lax.rem(me, 2)
    queries = pltpu.make_async_copy(q_ref, qlocal, ql_s)
    queries.start()
    lens = pltpu.make_async_copy(len_hbm, len_ref, len_s)
    lens.start()
    local = pltpu.make_async_copy(kv_ref.at[:, :, 0], kvlocal, loc_s)
    local.start()

    bar = pltpu.get_barrier_semaphore()
    peers = [me + 1 - 2 * core]
    for s in (SZ, SY, SX):
        for d in (1, 2, 3):
            t = shifted(me, s, d)
            peers += [t, t + 1 - 2 * core]
    for t in peers:
        pl.semaphore_signal(bar, inc=1, device_id={'dcp': t}, device_id_type=MESH)
    perm = onehot((192, 128), by_set)
    queries.wait()
    rows = jnp.dot(perm, qlocal[...].reshape(2 * BATCH, WIDTH), preferred_element_type=F32).astype(BF16)
    qsend[:, :, :, pl.ds(0, LATENT)] = rows[:, :LATENT].reshape(3, 8, 8, LATENT)
    rope2 = jnp.concatenate([rows[:, LATENT:], rows[:, LATENT:]], axis=1)
    qsend[:, :, :, pl.ds(LATENT, 2 * ROPE)] = rope2.reshape(3, 8, 8, 2 * ROPE)
    pl.semaphore_wait(bar, len(peers))
    own = [coord(me, RING[k]) * 2 + core for k in range(3)]

    def ring_dest(k, d, flip):
        dev = shifted(me, RING[k], d)
        dcore = core
        if flip:
            dev = dev + 1 - 2 * core
            dcore = 1 - core
        return dev, coord(dev, RING[k]) * 2 + dcore

    others = [(1, 0), (3, 0), (2, 0), (1, 1), (3, 1), (2, 1), (0, 1)]

    for k in range(3):
        for d, flip in others:
            dev, o = ring_dest(k, d, flip)
            remote(qsend.at[k, o], q0buf.at[k, own[k]], q0_s.at[k], q0_r.at[k], dev).start()
        q0buf[k, own[k]] = qsend[k, own[k]]

    def latent(b):
        return kv_ref.at[b, :, 0, :, pl.ds(0, LATENT)]

    def send_cache(t, which):
        k, i = t % 3, t // 3
        for d, flip in which:
            dev, o = ring_dest(k, d, flip)
            remote(latent(BASE[k] + o * COUNT[k] + i), kvbuf.at[t, own[k]], kv_s.at[t], kv_r.at[t], dev).start()
    for t in range(3):
        send_cache(t, others[:2] + others[3:5])
    send_cache(2, [(2, 0), (2, 1), (0, 1)])
    big = [coord(me, BIG[k]) for k in range(3)]
    small = [coord(me, SMALL[k]) for k in range(3)]
    for k in range(3):
        n = COUNT[k]
        remote(qsend.at[k, pl.ds(0, 7)], q0buf.at[k, pl.ds(0, 7)], q0_s.at[k], q0_r.at[k], me).wait_recv()
        order = onehot((n * 16, 64), lambda r, c: c == (((r & 15) >> 1) << 3) + ((r >> 4) << 1) + (r & 1))
        piece = jnp.dot(order, q0buf[k].reshape(64, QW), preferred_element_type=F32).astype(BF16)
        qbuf[k, pl.ds(0, n), big[k], small[k]] = piece.reshape(n, 16, QW)
        view = qbuf.at[k, pl.ds(0, n), big[k], small[k]]
        for d in (1, 3, 2):
            dev = shifted(me, SMALL[k] if LAST_BIG[k] else BIG[k], d)
            remote(view, view, q1_s.at[k], q1_r.at[k], dev).start()
    for t in range(2):
        send_cache(t, [(2, 0), (2, 1), (0, 1)])

    def block(k, idx, lo, cnt):
        n = COUNT[k]
        if LAST_BIG[k]:
            return qbuf.at[k, pl.ds(0, n), idx, pl.ds(lo, cnt)]
        return qbuf.at[k, pl.ds(0, n), pl.ds(lo, cnt), idx]
    mid = [big[k] if LAST_BIG[k] else small[k] for k in range(3)]
    axis = [BIG[k] if LAST_BIG[k] else SMALL[k] for k in range(3)]
    for k in range(3):
        three = block(k, 0, 0, 3)
        remote(three, three, q1_s.at[k], q1_r.at[k], me).wait_recv()
        view = block(k, mid[k], 0, 4)
        for j, d in enumerate((1, 3)):
            remote(view, view, q2_s.at[k, j], q2_r.at[k, j], shifted(me, axis[k], d)).start()
    local.wait()
    def pack(b, carry):
        ropes[b] = jnp.concatenate([kvlocal[b, 0, :, pl.ds(LATENT, ROPE)], kvlocal[b, 1, :, pl.ds(LATENT, ROPE)]], axis=1)
        return carry

    lax.fori_loop(0, BATCH, pack, 0, unroll=4)
    for k in range(3):
        n = COUNT[k]
        for d, flip in others:
            dev, o = ring_dest(k, d, flip)
            remote(ropes.at[pl.ds(BASE[k] + o * n, n)], kvrope.at[k, own[k], pl.ds(0, n)], kr_s.at[k], kr_r.at[k], dev).start()
        kvrope[k, own[k], pl.ds(0, n)] = ropes[pl.ds(BASE[k] + own[k] * n, n)]

    send_cache(3, others)
    send_cache(4, others[:2])
    send_cache(5, others[:2])

    def forward(k):
        for j, d in enumerate((1, 3)):
            whole = block(k, mid[k], 0, 4)
            remote(whole, whole, q2_s.at[k, j], q2_r.at[k, j], me).wait_recv()
            half = block(k, lax.rem(mid[k] + (3 if j == 0 else 1), 4), 2 * j, 2)
            remote(half, half, q3_s.at[k, j], q3_r.at[k, j], shifted(me, axis[k], d)).start()
    forward(2)
    send_cache(4, others[2:])
    send_cache(6, others)
    send_cache(7, others)
    forward(0)
    forward(1)
    send_cache(5, others[2:])
    for t in range(SLOTS):
        k, i = t % 3, t // 3
        pltpu.make_async_copy(latent(BASE[k] + own[k] * COUNT[k] + i), kvbuf.at[t, own[k]], kv_l.at[t]).start()

    lens.wait()
    for k in range(3):
        n = COUNT[k]
        for j in range(2):
            half = block(k, mid[k], 0, 2)
            remote(half, half, q3_s.at[k, j], q3_r.at[k, j], me).wait_recv()
        seven = kvrope.at[k, pl.ds(0, 7), pl.ds(0, n)]
        remote(seven, seven, kr_s.at[k], kr_r.at[k], me).wait_recv()
    def attend(t, carry):
        k = lax.rem(t, 3)
        i = lax.div(t, 3)
        ring = pick(k, RING)
        u = coord(me, ring)
        bstride = pick(k, BIG)
        b_me = coord(me, bstride)
        length = len_ref[24 * k + (u * 2 + core) * pick(k, COUNT) + i]
        pltpu.make_async_copy(latent(0), kvbuf.at[t, 0], kv_l.at[t]).wait()
        seven = kvbuf.at[t, pl.ds(0, 7)]
        remote(seven, seven, kv_s.at[t], kv_r.at[t], me).wait_recv()
        q = qbuf[k, i].reshape(256, QW)
        keys = kvbuf[t].reshape(1024, LATENT)
        packed = kvrope[k, :, i]
        lane = lax.broadcasted_iota(jnp.int32, packed.shape, 2)
        zero = jnp.zeros_like(packed)
        rope = jnp.stack([jnp.where(lane < ROPE, packed, zero), jnp.where(lane >= ROPE, packed, zero)], axis=1).reshape(1024, 2 * ROPE)
        nt = (((1,), (1,)), ((), ()))
        s = lax.dot_general(q[:, :LATENT], keys, nt, preferred_element_type=F32)
        s = s + lax.dot_general(q[:, LATENT:], rope, nt, preferred_element_type=F32)
        s = s * SCALE
        kk = lax.broadcasted_iota(jnp.int32, (1, 1024), 1)
        dsrc = (me - u * ring - core) + (kk >> 8) * ring + ((kk >> 7) & 1)
        pos = (((kk >> 6) & 1) * GROUP + dsrc) * PAGE + (kk & 63)
        tok = lax.broadcasted_iota(jnp.int32, (256, 1), 0) & 1
        s = jnp.where(pos - tok <= length - 2, s, MASKED)
        m = jnp.max(s, axis=1, keepdims=True)
        w = jnp.exp(s - m)
        l = jnp.sum(w, axis=1, keepdims=True)
        part = jnp.dot(w.astype(BF16), keys, preferred_element_type=F32)
        obuf[k, i] = (part * (1.0 / l)).astype(BF16).reshape(4, 4, 16, LATENT)
        l1send[k, i] = tile_lse((m + jnp.log(l)).reshape(4, 4, 16, 1))
        for d in (1, 3, 2):
            b = lax.rem(b_me + d, 4)
            remote(obuf.at[k, i, b], r1buf.at[k, i, b_me], r1_s.at[t], r1_r.at[t], me + (b - b_me) * bstride).start()
            remote(l1send.at[k, i, b], l1recv.at[k, i, b_me], l1_s.at[t], l1_r.at[t], me + (b - b_me) * bstride).start()
        r1buf[k, i, b_me] = obuf[k, i, b_me]
        l1recv[k, i, b_me] = l1send[k, i, b_me]
        return carry

    lax.fori_loop(0, SLOTS, attend, 0)

    def merge(lse, ref):
        top = jnp.max(lse, axis=0)
        e = jnp.exp(lse - top[None])
        total = jnp.sum(e, axis=0)
        wgt = e / total[None]
        acc = wgt[0] * ref[0].astype(F32)
        for p in range(1, 4):
            acc = acc + wgt[p] * ref[p].astype(F32)
        return acc.astype(BF16), top + jnp.log(total)

    lacc = [jnp.zeros((4, 16, 128), F32) for _ in range(3)]
    for t in (0, 2, 1, 3, 5, 4, 6, 7):
        k, i = t % 3, t // 3
        three = l1recv.at[k, i, pl.ds(0, 3)]
        remote(three, three, l1_s.at[t], l1_r.at[t], me).wait_recv()
        three = r1buf.at[k, i, pl.ds(0, 3)]
        remote(three, three, r1_s.at[t], r1_r.at[t], me).wait_recv()
        both, lse = merge(untile_lse(l1recv[k, i].astype(F32)), r1buf.at[k, i])
        m1buf[k, i] = both
        lacc[k] = put_lse(lacc[k], lse, i)
        for d in (1, 3, 2):
            b = lax.rem(small[k] + d, 4)
            remote(m1buf.at[k, i, b], r2buf.at[k, i, small[k]], r2_s.at[t], r2_r.at[t], shifted(me, SMALL[k], d)).start()
        r2buf[k, i, small[k]] = m1buf[k, i, small[k]]
        if i == COUNT[k] - 1:
            l2send[k] = lacc[k].astype(BF16)
            for d in (1, 3, 2):
                b = lax.rem(small[k] + d, 4)
                remote(l2send.at[k, b], l2recv.at[k, small[k]], l2_s.at[k], l2_r.at[k], shifted(me, SMALL[k], d)).start()
            l2recv[k, small[k]] = l2send[k, small[k]]

    for k in (2, 0, 1):
        n = COUNT[k]
        three = l2recv.at[k, pl.ds(0, 3)]
        remote(three, three, l2_s.at[k], l2_r.at[k], me).wait_recv()
        lr = l2recv[k].astype(F32)
        merged = []
        for i in range(n):
            t = 3 * i + k
            three = r2buf.at[k, i, pl.ds(0, 3)]
            remote(three, three, r2_s.at[t], r2_r.at[t], me).wait_recv()
            merged.append(merge(get_lse(lr, i), r2buf.at[k, i])[0])
        order = onehot((64, n * 16), lambda r, c: r == (((c & 15) >> 1) << 3) + ((c >> 4) << 1) + (c & 1))
        out = jnp.dot(order, jnp.concatenate(merged, axis=0), preferred_element_type=F32)
        fsend[k] = out.astype(BF16).reshape(8, 8, LATENT)
        for d, flip in others:
            dev, o = ring_dest(k, d, flip)
            remote(fsend.at[k, o], frecv.at[k, own[k]], f_s.at[k], f_r.at[k], dev).start()
        frecv[k, own[k]] = fsend[k, own[k]]
    back = onehot((128, 192), lambda r, c: by_set(c, r))
    for k in range(3):
        seven = frecv.at[k, pl.ds(0, 7)]
        remote(seven, seven, f_s.at[k], f_r.at[k], me).wait_recv()
    out = jnp.dot(back, frecv[...].reshape(192, LATENT), preferred_element_type=F32)
    out_ref[...] = out.astype(BF16).reshape(BATCH, 2, LATENT)
    def sent(view, sem):
        remote(view, view, sem, sem, me).wait_send()

    for t in range(SLOTS):
        k, i = t % 3, t // 3
        sent(kvbuf.at[t, pl.ds(0, 7)], kv_s.at[t])
        sent(r1buf.at[k, i, pl.ds(0, 3)], r1_s.at[t])
        sent(r2buf.at[k, i, pl.ds(0, 3)], r2_s.at[t])
        sent(l1recv.at[k, i, pl.ds(0, 3)], l1_s.at[t])
    for k in range(3):
        n = COUNT[k]
        sent(q0buf.at[k, pl.ds(0, 7)], q0_s.at[k])
        sent(block(k, 0, 0, 3), q1_s.at[k])
        for j in range(2):
            sent(block(k, 0, 0, 4), q2_s.at[k, j])
            sent(block(k, 0, 0, 2), q3_s.at[k, j])
        sent(kvrope.at[k, pl.ds(0, 7), pl.ds(0, n)], kr_s.at[k])
        sent(l2recv.at[k, pl.ds(0, 3)], l2_s.at[k])
        sent(frecv.at[k, pl.ds(0, 7)], f_s.at[k])


def solution(mesh):
    def local_step(q_blk, kv_blk, len_blk):
        dma = pltpu.SemaphoreType.DMA
        vmem = pltpu.VMEM

        def hbm(v):
            return pltpu.with_memory_space_constraint(v, pltpu.HBM)

        out = pl.pallas_call(
            kernel,
            out_shape=jax.ShapeDtypeStruct((BATCH, 2, LATENT), BF16),
            in_specs=[
                pl.BlockSpec(memory_space=pltpu.HBM),
                pl.BlockSpec(memory_space=pltpu.HBM),
                pl.BlockSpec(memory_space=pltpu.HBM),
            ],
            out_specs=pl.BlockSpec(memory_space=pltpu.VMEM),
            scratch_shapes=[
                pltpu.SMEM((BATCH,), jnp.int32),
                vmem((BATCH, 2, WIDTH), BF16),
                vmem((BATCH, 2, PAGE, WIDTH), BF16),
                vmem((BATCH, PAGE, 2 * ROPE), BF16),
                vmem((SLOTS, 8, 2, PAGE, LATENT), BF16),
                vmem((3, 8, 3, PAGE, 2 * ROPE), BF16),
                vmem((3, 8, 8, QW), BF16),
                vmem((3, 8, 8, QW), BF16),
                vmem((3, 3, 4, 4, 16, QW), BF16),
                vmem((3, 3, 4, 4, 16, LATENT), BF16),
                vmem((3, 3, 4, 4, 16, LATENT), BF16),
                vmem((3, 3, 4, 16, LATENT), BF16),
                vmem((3, 3, 4, 16, LATENT), BF16),
                vmem((3, 3, 4, 16, 128), BF16),
                vmem((3, 3, 4, 16, 128), BF16),
                vmem((3, 4, 16, 128), BF16),
                vmem((3, 4, 16, 128), BF16),
                vmem((3, 8, 8, LATENT), BF16),
                vmem((3, 8, 8, LATENT), BF16),
                dma, dma, dma,
                dma((SLOTS,)), dma((SLOTS,)), dma((SLOTS,)),
                dma((3,)), dma((3,)),
                dma((3,)), dma((3,)),
                dma((3,)), dma((3,)),
                dma((3, 2)), dma((3, 2)),
                dma((3, 2)), dma((3, 2)),
                dma((SLOTS,)), dma((SLOTS,)),
                dma((SLOTS,)), dma((SLOTS,)),
                dma((SLOTS,)), dma((SLOTS,)),
                dma((3,)), dma((3,)),
                dma((3,)), dma((3,)),
            ],
            compiler_params=pltpu.CompilerParams(collective_id=0, has_side_effects=True, vmem_limit_bytes=44 * 1024 * 1024),
            name='mla',
        )(hbm(len_blk), hbm(q_blk.reshape(BATCH, 2, WIDTH)), kv_blk)
        return out.reshape(BATCH, 2, 1, LATENT)

    return jax.shard_map(local_step, mesh=mesh, in_specs=(P('dp', None, 'dcp', None), P('dp', None, 'dcp', None, None), P('dp')), out_specs=P('dp', None, 'dcp', None), check_vma=False)
```

```python
import jax
import jax.numpy as jnp
from jax import lax
from jax.experimental import pallas as pl
from jax.experimental.pallas import tpu as pltpu
from jax.sharding import PartitionSpec as P

LATENT = 512
ROPE = 64
NOPE = 128
WIDTH = LATENT + ROPE
QW = 2 * LATENT + 2 * ROPE
PAGE = 64
GROUP = 128
BATCH = 64
MASKED = -1e30
SCALE = (NOPE + ROPE) ** -0.5
MESH = pl.DeviceIdType.MESH
BF16 = jnp.bfloat16
F32 = jnp.float32

SZ, SY, SX = 32, 8, 2
RING = (SZ, SY, SX)
BIG = (SX, SZ, SY)
SMALL = (SY, SX, SZ)
COUNT = (3, 3, 2)
BASE = (0, 24, 48)
SLOTS = 8
LATE = 7
UNITS = ((0, 0, 3, True), (1, 0, 3, False), (2, 0, 1, True), (2, 1, 1, False))


def pick(k, vals):
    return jnp.where(k == 0, vals[0], jnp.where(k == 1, vals[1], vals[2]))


def coord(me, stride):
    return lax.rem(lax.div(me, stride), 4)


def shifted(me, stride, d):
    c = coord(me, stride)
    return me + (lax.rem(c + d, 4) - c) * stride


def remote(src, dst, ssem, rsem, dev):
    return pltpu.make_async_remote_copy(src_ref=src, dst_ref=dst, send_sem=ssem, recv_sem=rsem, device_id={'dcp': dev}, device_id_type=MESH)


def arrived(view, sem):
    pltpu.make_async_copy(view, view, sem).wait()


def split3(v):
    hi = v.astype(BF16).astype(F32)
    mid = (v - hi).astype(BF16).astype(F32)
    return hi, mid, v - hi - mid


def put_lse(old, lse, i):
    lane = lax.broadcasted_iota(jnp.int32, old.shape, len(old.shape) - 1)
    hi, mid, lo = split3(lse)
    return jnp.where(lane == i, hi, jnp.where(lane == 8 + i, mid, jnp.where(lane == 16 + i, lo, old)))


def tile_lse(lse):
    tile = jnp.zeros((4, 16, 128), F32)
    lane = lax.broadcasted_iota(jnp.int32, tile.shape, 2)
    for b in range(4):
        for j, v in enumerate(split3(lse[:, b])):
            tile = jnp.where(lane == 32 * b + j, v, tile)
    return tile.astype(BF16)


def untile_lse(x):
    return jnp.stack([x[..., 32 * b:32 * b + 1] + x[..., 32 * b + 1:32 * b + 2] + x[..., 32 * b + 2:32 * b + 3] for b in range(4)], axis=1)


def get_lse(x, i):
    return x[..., i:i + 1] + x[..., 8 + i:9 + i] + x[..., 16 + i:17 + i]


def onehot(shape, fn):
    row = lax.broadcasted_iota(jnp.int32, shape, 0)
    col = lax.broadcasted_iota(jnp.int32, shape, 1)
    return jnp.where(fn(row, col), 1.0, 0.0).astype(BF16)


def by_set(rows, cols, pad, tokens, tok):
    hit = None
    for k in range(3):
        n = COUNT[k]
        r = rows - k * 8 * pad
        o, j = lax.div(jnp.maximum(r, 0), pad), r & (pad - 1)
        m = (r >= 0) & (r < 8 * pad) & (j < n * tokens) & (cols == 2 * (BASE[k] + o * n) + (2 // tokens) * j + tok)
        hit = m if hit is None else hit | m
    return hit


def kernel(len_hbm, q_ref, kv_ref, out_ref, len_ref, qlocal, kvlocal, ropes, kvbuf, kvrope, qsend, q0buf, qbuf, obuf, r1buf, m1buf, r2buf,
           l1send, l1recv, l2send, l2recv, dbuf, dlse, fsend, frecv,
           len_s, ql_s, loc_s, kv_s, kv_r, kv_l, kr_s, kr_r, q0_s, q0_r, q1_s, q1_r, q2_s, q2_r, q3_s, q3_r, r1_s, r1_r, r2_s, r2_r,
           l1_s, l1_r, l2_s, l2_r, d_s, d_r, dl_s, dl_r, f_s, f_r):
    me = lax.axis_index('dcp')
    core = lax.rem(me, 2)
    queries = pltpu.make_async_copy(q_ref, qlocal, ql_s)
    queries.start()
    lens = pltpu.make_async_copy(len_hbm, len_ref, len_s)
    lens.start()
    local = pltpu.make_async_copy(kv_ref.at[:, :, 0], kvlocal, loc_s)
    local.start()

    bar = pltpu.get_barrier_semaphore()
    peers = [me + 1 - 2 * core]
    for s in (SZ, SY, SX):
        for d in (1, 2, 3):
            t = shifted(me, s, d)
            peers += [t, t + 1 - 2 * core]
    for d1 in (1, 2, 3):
        for d2 in (1, 2, 3):
            peers.append(shifted(shifted(me, BIG[1], d1), SMALL[1], d2))
    for t in peers:
        pl.semaphore_signal(bar, inc=1, device_id={'dcp': t}, device_id_type=MESH)
    perms = [onehot((96, 128), lambda r, c, tok=tok: by_set(r, c, 4, 1, tok)) for tok in range(2)]
    queries.wait()
    both = [jnp.dot(perm, qlocal[...].reshape(2 * BATCH, WIDTH), preferred_element_type=F32).astype(BF16) for perm in perms]
    for tok in range(2):
        qsend[:, :, :, pl.ds(tok * LATENT, LATENT)] = both[tok][:, :LATENT].reshape(3, 8, 4, LATENT)
    rotary = jnp.concatenate([both[0][:, LATENT:], both[1][:, LATENT:]], axis=1)
    qsend[:, :, :, pl.ds(2 * LATENT, 2 * ROPE)] = rotary.reshape(3, 8, 4, 2 * ROPE)
    pl.semaphore_wait(bar, len(peers))
    own = [coord(me, RING[k]) * 2 + core for k in range(3)]

    def ring_dest(k, d, flip):
        dev = shifted(me, RING[k], d)
        dcore = core
        if flip:
            dev = dev + 1 - 2 * core
            dcore = 1 - core
        return dev, coord(dev, RING[k]) * 2 + dcore

    others = [(1, 0), (3, 0), (2, 0), (1, 1), (3, 1), (2, 1), (0, 1)]

    for k in range(3):
        for d, flip in others:
            dev, o = ring_dest(k, d, flip)
            remote(qsend.at[k, o], q0buf.at[k, own[k]], q0_s, q0_r, dev).start()
        q0buf[k, own[k]] = qsend[k, own[k]]

    def latent(b):
        return kv_ref.at[b, :, 0, :, pl.ds(0, LATENT)]

    def send_cache(t, which):
        k, i = t % 3, t // 3
        for d, flip in which:
            dev, o = ring_dest(k, d, flip)
            remote(latent(BASE[k] + o * COUNT[k] + i), kvbuf.at[t, own[k]], kv_s, kv_r.at[t], dev).start()
    for t in range(3):
        send_cache(t, others[:2] + others[3:5])
    send_cache(2, [(2, 0), (2, 1), (0, 1)])
    big = [coord(me, BIG[k]) for k in range(3)]
    small = [coord(me, SMALL[k]) for k in range(3)]
    arrived(q0buf.at[:, pl.ds(0, 7)], q0_r)
    for k in range(3):
        n = COUNT[k]
        order = onehot((n * 8, 32), lambda r, c: c == ((r & 7) << 2) + (r >> 3))
        piece = jnp.dot(order, q0buf[k].reshape(32, QW), preferred_element_type=F32).astype(BF16)
        qbuf[k, pl.ds(0, n), big[k], small[k]] = piece.reshape(n, 8, QW)
    for j, (k, i, n, last_big) in enumerate(UNITS):
        view = qbuf.at[k, pl.ds(i, n), big[k], small[k]]
        for d in (1, 3, 2):
            dev = shifted(me, SMALL[k] if last_big else BIG[k], d)
            remote(view, view, q1_s, q1_r.at[j], dev).start()
    for t in range(2):
        send_cache(t, [(2, 0), (2, 1), (0, 1)])

    def block(u, idx, lo, cnt):
        k, i, n, last_big = UNITS[u]
        if last_big:
            return qbuf.at[k, pl.ds(i, n), idx, pl.ds(lo, cnt)]
        return qbuf.at[k, pl.ds(i, n), pl.ds(lo, cnt), idx]

    mid = [big[k] if last_big else small[k] for k, i, n, last_big in UNITS]
    axis = [BIG[k] if last_big else SMALL[k] for k, i, n, last_big in UNITS]
    for u in range(4):
        arrived(block(u, 0, 0, 3), q1_r.at[u])
        view = block(u, mid[u], 0, 4)
        for j, d in enumerate((1, 3)):
            remote(view, view, q2_s, q2_r.at[u, j], shifted(me, axis[u], d)).start()
    local.wait()
    def pack(b, carry):
        ropes[b] = jnp.concatenate([kvlocal[b, 0, :, pl.ds(LATENT, ROPE)], kvlocal[b, 1, :, pl.ds(LATENT, ROPE)]], axis=1)
        return carry

    lax.fori_loop(0, BATCH, pack, 0, unroll=4)
    for k in range(3):
        n = COUNT[k]
        for d, flip in others:
            dev, o = ring_dest(k, d, flip)
            remote(ropes.at[pl.ds(BASE[k] + o * n, n)], kvrope.at[k, own[k], pl.ds(0, n)], kr_s, kr_r, dev).start()
        kvrope[k, own[k], pl.ds(0, n)] = ropes[pl.ds(BASE[k] + own[k] * n, n)]

    send_cache(3, others)
    send_cache(4, others[:2])
    send_cache(5, others[:2])

    def forward(k):
        for j, d in enumerate((1, 3)):
            arrived(block(k, mid[k], 0, 4), q2_r.at[k, j])
            half = block(k, lax.rem(mid[k] + (3 if j == 0 else 1), 4), 2 * j, 2)
            remote(half, half, q3_s, q3_r, shifted(me, axis[k], d)).start()
    forward(2)
    forward(3)
    send_cache(4, others[2:])
    send_cache(6, others)
    send_cache(7, others)
    forward(0)
    forward(1)
    send_cache(5, others[2:])
    for t in range(SLOTS):
        k, i = t % 3, t // 3
        pltpu.make_async_copy(latent(BASE[k] + own[k] * COUNT[k] + i), kvbuf.at[t, own[k]], kv_l).start()

    lens.wait()
    arrived(qbuf.at[pl.ds(0, 2), 0], q3_r)
    arrived(ropes.at[pl.ds(0, 56)], kr_r)
    arrived(kvbuf.at[:, 0], kv_l)
    def attend(t, carry):
        k = lax.rem(t, 3)
        i = lax.div(t, 3)
        ring = pick(k, RING)
        u = coord(me, ring)
        bstride = pick(k, BIG)
        b_me = coord(me, bstride)
        length = len_ref[24 * k + (u * 2 + core) * pick(k, COUNT) + i]
        arrived(kvbuf.at[t, pl.ds(0, 7)], kv_r.at[t])
        q2 = qbuf[k, i].reshape(128, QW)
        q = jnp.concatenate([q2[:, :LATENT], q2[:, LATENT:2 * LATENT]], axis=0)
        pair = q2[:, 2 * LATENT:]
        swapped = jnp.concatenate([pair[:, ROPE:], pair[:, :ROPE]], axis=1)
        low = lax.broadcasted_iota(jnp.int32, pair.shape, 1) < ROPE
        qr = jnp.concatenate([jnp.where(low, pair, swapped), jnp.where(low, swapped, pair)], axis=0)
        keys = kvbuf[t].reshape(1024, LATENT)
        packed = kvrope[k, :, i]
        lane = lax.broadcasted_iota(jnp.int32, packed.shape, 2)
        zero = jnp.zeros_like(packed)
        rope = jnp.stack([jnp.where(lane < ROPE, packed, zero), jnp.where(lane >= ROPE, packed, zero)], axis=1).reshape(1024, 2 * ROPE)
        nt = (((1,), (1,)), ((), ()))
        s = lax.dot_general(q, keys, nt, preferred_element_type=F32)
        s = s + lax.dot_general(qr, rope, nt, preferred_element_type=F32)
        s = s * SCALE
        kk = lax.broadcasted_iota(jnp.int32, (1, 1024), 1)
        dsrc = (me - u * ring - core) + (kk >> 8) * ring + ((kk >> 7) & 1)
        pos = (((kk >> 6) & 1) * GROUP + dsrc) * PAGE + (kk & 63)
        tok = lax.broadcasted_iota(jnp.int32, (256, 1), 0) >> 7
        s = jnp.where(pos - tok <= length - 2, s, MASKED)
        m = jnp.max(s, axis=1, keepdims=True)
        w = jnp.exp(s - m)
        l = jnp.sum(w, axis=1, keepdims=True)
        part = jnp.dot(w.astype(BF16), keys, preferred_element_type=F32)
        part = (part * (1.0 / l)).astype(BF16)
        obuf[k, i, :, :, pl.ds(0, 8)] = part[:128].reshape(4, 4, 8, LATENT)
        obuf[k, i, :, :, pl.ds(8, 8)] = part[128:].reshape(4, 4, 8, LATENT)
        lse = m + jnp.log(l)
        l1send[k, i] = tile_lse(jnp.concatenate([lse[:128].reshape(4, 4, 8, 1), lse[128:].reshape(4, 4, 8, 1)], axis=2))

        @pl.when(t < LATE)
        def _():
            for d in (1, 3, 2):
                b = lax.rem(b_me + d, 4)
                dev = me + (b - b_me) * bstride
                remote(obuf.at[k, i, b], r1buf.at[t, b_me], r1_s, r1_r.at[t], dev).start()
                remote(l1send.at[k, i, b], l1recv.at[t, b_me], l1_s, l1_r.at[t], dev).start()
            r1buf[t, b_me] = obuf[k, i, b_me]
            l1recv[t, b_me] = l1send[k, i, b_me]

        @pl.when(t == LATE)
        def _():
            place = big[1] * 4 + small[1]
            for d1, d2 in ((1, 0), (3, 0), (0, 1), (0, 3), (1, 1), (1, 3), (3, 1), (3, 3), (2, 0), (0, 2), (1, 2), (3, 2), (2, 1), (2, 3), (2, 2)):
                b1, b2 = lax.rem(big[1] + d1, 4), lax.rem(small[1] + d2, 4)
                dev = me + (b1 - big[1]) * BIG[1] + (b2 - small[1]) * SMALL[1]
                remote(obuf.at[1, 2, b1, b2], dbuf.at[place], d_s, d_r, dev).start()
                remote(l1send.at[1, 2, b1], dlse.at[place], dl_s, dl_r, dev).start()
            dbuf[place] = obuf[1, 2, big[1], small[1]]
            dlse[place] = l1send[1, 2, big[1]]
        return carry

    lax.fori_loop(0, SLOTS, attend, 0)

    def merge(lse, ref):
        top = jnp.max(lse, axis=0)
        e = jnp.exp(lse - top[None])
        total = jnp.sum(e, axis=0)
        wgt = e / total[None]
        acc = wgt[0] * ref[0].astype(F32)
        for p in range(1, ref.shape[0]):
            acc = acc + wgt[p] * ref[p].astype(F32)
        return acc.astype(BF16), top + jnp.log(total)

    lacc = [jnp.zeros((4, 16, 128), F32) for _ in range(3)]
    for t in (0, 2, 1, 3, 5, 4, 6):
        k, i = t % 3, t // 3
        arrived(l1recv.at[t, pl.ds(0, 3)], l1_r.at[t])
        arrived(r1buf.at[t, pl.ds(0, 3)], r1_r.at[t])
        both, lse = merge(untile_lse(l1recv[t].astype(F32)), r1buf.at[t])
        m1buf[k, i] = both
        lacc[k] = put_lse(lacc[k], lse, i)
        for d in (1, 3, 2):
            b = lax.rem(small[k] + d, 4)
            remote(m1buf.at[k, i, b], r2buf.at[t, small[k]], r2_s, r2_r.at[k], shifted(me, SMALL[k], d)).start()
        r2buf[t, small[k]] = m1buf[k, i, small[k]]
        if t >= 4:
            l2send[k] = lacc[k].astype(BF16)
            for d in (1, 3, 2):
                b = lax.rem(small[k] + d, 4)
                remote(l2send.at[k, b], l2recv.at[k, small[k]], l2_s, l2_r.at[k], shifted(me, SMALL[k], d)).start()
            l2recv[k, small[k]] = l2send[k, small[k]]

    for k in (2, 0, 1):
        n = COUNT[k]
        if k == LATE % 3:
            arrived(dlse.at[pl.ds(0, 15)], dl_r)
            arrived(dbuf.at[pl.ds(0, 15)], d_r)
            x = dlse[...].astype(F32)
            lse = jnp.zeros((16, 16, 1), F32)
            for b in range(4):
                v = x[..., 32 * b:32 * b + 1] + x[..., 32 * b + 1:32 * b + 2] + x[..., 32 * b + 2:32 * b + 3]
                lse = jnp.where(small[k] == b, v, lse)
            late = merge(lse, dbuf)[0]
        arrived(l2recv.at[k, pl.ds(0, 3)], l2_r.at[k])
        arrived(r2buf.at[pl.ds(0, n if k != LATE % 3 else n - 1), pl.ds(0, 3)], r2_r.at[k])
        lr = l2recv[k].astype(F32)
        merged = []
        for i in range(n):
            t = 3 * i + k
            if t == LATE:
                merged.append(late)
                continue
            merged.append(merge(get_lse(lr, i), r2buf.at[t])[0])
        order = onehot((64, n * 16), lambda r, c: r == ((c & 7) << 3) + ((c >> 4) << 1) + ((c >> 3) & 1))
        out = jnp.dot(order, jnp.concatenate(merged, axis=0), preferred_element_type=F32)
        fsend[k] = out.astype(BF16).reshape(8, 8, LATENT)
        for d, flip in others:
            dev, o = ring_dest(k, d, flip)
            remote(fsend.at[k, o], frecv.at[k, own[k]], f_s, f_r, dev).start()
        frecv[k, own[k]] = fsend[k, own[k]]
    back = onehot((128, 192), lambda r, c: by_set(c, r, 8, 2, 0))
    arrived(frecv.at[:, pl.ds(0, 7)], f_r)
    out = jnp.dot(back, frecv[...].reshape(192, LATENT), preferred_element_type=F32)
    out_ref[...] = out.astype(BF16).reshape(BATCH, 2, LATENT)
    def sent(view, sem):
        remote(view, view, sem, sem, me).wait_send()

    sent(q0buf.at[:, pl.ds(0, 7)], q0_s)
    sent(qbuf.at[pl.ds(0, 2), :, :, 0], q1_s)
    sent(qbuf.at[pl.ds(0, 2), pl.ds(0, 2)], q2_s)
    sent(qbuf.at[pl.ds(0, 2), 0], q3_s)
    sent(ropes.at[pl.ds(0, 56)], kr_s)
    sent(kvbuf.at[:, pl.ds(0, 7)], kv_s)
    sent(r1buf.at[pl.ds(0, LATE), pl.ds(0, 3)], r1_s)
    sent(l1recv.at[pl.ds(0, LATE), pl.ds(0, 3)], l1_s)
    sent(r2buf.at[pl.ds(0, LATE), pl.ds(0, 3)], r2_s)
    sent(l2recv.at[:, pl.ds(0, 3)], l2_s)
    sent(dbuf.at[pl.ds(0, 15)], d_s)
    sent(dlse.at[pl.ds(0, 15)], dl_s)
    sent(frecv.at[:, pl.ds(0, 7)], f_s)


def solution(mesh):
    def local_step(q_blk, kv_blk, len_blk):
        dma = pltpu.SemaphoreType.DMA
        vmem = pltpu.VMEM

        def hbm(v):
            return pltpu.with_memory_space_constraint(v, pltpu.HBM)

        out = pl.pallas_call(
            kernel,
            out_shape=jax.ShapeDtypeStruct((BATCH, 2, LATENT), BF16),
            in_specs=[
                pl.BlockSpec(memory_space=pltpu.HBM),
                pl.BlockSpec(memory_space=pltpu.HBM),
                pl.BlockSpec(memory_space=pltpu.HBM),
            ],
            out_specs=pl.BlockSpec(memory_space=pltpu.VMEM),
            scratch_shapes=[
                pltpu.SMEM((BATCH,), jnp.int32),
                vmem((BATCH, 2, WIDTH), BF16),
                vmem((BATCH, 2, PAGE, WIDTH), BF16),
                vmem((BATCH, PAGE, 2 * ROPE), BF16),
                vmem((SLOTS, 8, 2, PAGE, LATENT), BF16),
                vmem((3, 8, 3, PAGE, 2 * ROPE), BF16),
                vmem((3, 8, 4, QW), BF16),
                vmem((3, 8, 4, QW), BF16),
                vmem((3, 3, 4, 4, 8, QW), BF16),
                vmem((3, 3, 4, 4, 16, LATENT), BF16),
                vmem((SLOTS, 4, 4, 16, LATENT), BF16),
                vmem((3, 3, 4, 16, LATENT), BF16),
                vmem((SLOTS, 4, 16, LATENT), BF16),
                vmem((3, 3, 4, 16, 128), BF16),
                vmem((SLOTS, 4, 16, 128), BF16),
                vmem((3, 4, 16, 128), BF16),
                vmem((3, 4, 16, 128), BF16),
                vmem((16, 16, LATENT), BF16),
                vmem((16, 16, 128), BF16),
                vmem((3, 8, 8, LATENT), BF16),
                vmem((3, 8, 8, LATENT), BF16),
                dma, dma, dma,
                dma, dma((SLOTS,)), dma,
                dma, dma,
                dma, dma,
                dma, dma((4,)),
                dma, dma((4, 2)),
                dma, dma,
                dma, dma((SLOTS,)),
                dma, dma((3,)),
                dma, dma((SLOTS,)),
                dma, dma((3,)),
                dma, dma, dma, dma,
                dma, dma,
            ],
            compiler_params=pltpu.CompilerParams(collective_id=0, has_side_effects=True, vmem_limit_bytes=44 * 1024 * 1024),
            name='mla',
        )(hbm(len_blk), hbm(q_blk.reshape(BATCH, 2, WIDTH)), kv_blk)
        return out.reshape(BATCH, 2, 1, LATENT)

    return jax.shard_map(local_step, mesh=mesh, in_specs=(P('dp', None, 'dcp', None), P('dp', None, 'dcp', None, None), P('dp')), out_specs=P('dp', None, 'dcp', None), check_vma=False)
```

```python
import jax
import jax.numpy as jnp
from jax import lax
from jax.experimental import pallas as pl
from jax.experimental.pallas import tpu as pltpu
from jax.sharding import PartitionSpec as P

LATENT = 512
ROPE = 64
NOPE = 128
WIDTH = LATENT + ROPE
QW = 2 * LATENT + 2 * ROPE
PAGE = 64
GROUP = 128
BATCH = 64
MASKED = -1e30
SCALE = (NOPE + ROPE) ** -0.5
MESH = pl.DeviceIdType.MESH
BF16 = jnp.bfloat16
F32 = jnp.float32

SZ, SY, SX = 32, 8, 2
RING = (SZ, SY, SX)
BIG = (SX, SZ, SY)
SMALL = (SY, SX, SZ)
COUNT = (3, 3, 2)
BASE = (0, 24, 48)
SLOTS = 8
STEPS = (1, 3, 2)
SENDS = (2, 1, 3)
UNITS = ((0, 0, 3, True), (1, 0, 3, False), (2, 0, 1, True), (2, 1, 1, True))


def pick(k, vals):
    return jnp.where(k == 0, vals[0], jnp.where(k == 1, vals[1], vals[2]))


def coord(me, stride):
    return lax.rem(lax.div(me, stride), 4)


def shifted(me, stride, d):
    c = coord(me, stride)
    return me + (lax.rem(c + d, 4) - c) * stride


def remote(src, dst, ssem, rsem, dev):
    return pltpu.make_async_remote_copy(src_ref=src, dst_ref=dst, send_sem=ssem, recv_sem=rsem, device_id={'dcp': dev}, device_id_type=MESH)


def arrived(view, sem):
    pltpu.make_async_copy(view, view, sem).wait()


def split3(v):
    hi = v.astype(BF16).astype(F32)
    mid = (v - hi).astype(BF16).astype(F32)
    return hi, mid, v - hi - mid


def put_lse(tile, lse, b):
    lane = lax.broadcasted_iota(jnp.int32, tile.shape, len(tile.shape) - 1)
    for j, v in enumerate(split3(lse)):
        tile = jnp.where(lane == 32 * b + j, v, tile)
    return tile


def get_lse(x, b):
    return sum(x[..., 32 * b + j:32 * b + j + 1] for j in range(3))


def tile_lse(lse):
    tile = jnp.zeros((4, 16, 128), F32)
    for b in range(4):
        tile = put_lse(tile, lse[:, b], b)
    return tile.astype(BF16)


def untile_lse(x):
    return jnp.stack([get_lse(x, b) for b in range(4)], axis=1)


def first(count):
    return pl.ds(0, count)


def onehot(shape, fn):
    row = lax.broadcasted_iota(jnp.int32, shape, 0)
    col = lax.broadcasted_iota(jnp.int32, shape, 1)
    return jnp.where(fn(row, col), 1.0, 0.0).astype(BF16)


def by_set(rows, cols, pad, tokens, tok):
    hit = None
    for k in range(3):
        n = COUNT[k]
        r = rows - k * 8 * pad
        o, j = lax.div(jnp.maximum(r, 0), pad), r & (pad - 1)
        m = (r >= 0) & (r < 8 * pad) & (j < n * tokens) & (cols == 2 * (BASE[k] + o * n) + (2 // tokens) * j + tok)
        hit = m if hit is None else hit | m
    return hit


def kernel(len_hbm, q_ref, kv_ref, out_ref, len_ref, qlocal, kvlocal, ropes, kvbuf, kvrope, qsend, q0buf, qbuf, obuf, r1buf, m1buf, r2buf,
           l1send, l1recv, l2send, l2recv, fsend, frecv,
           len_s, ql_s, loc_s, kv_s, kv_r, kv_l, kr_s, kr_r, q0_s, q0_r, q1_s, q1_r, q2_s, q2_r, q3_s, q3_r, r1_s, r1_r, r2_s, r2_r,
           l1_s, l1_r, l2_s, l2_r, f_s, f_r):
    me = lax.axis_index('dcp')
    core = lax.rem(me, 2)
    queries = pltpu.make_async_copy(q_ref, qlocal, ql_s)
    queries.start()
    lens = pltpu.make_async_copy(len_hbm, len_ref, len_s)
    lens.start()
    local = pltpu.make_async_copy(kv_ref.at[:, :, 0], kvlocal, loc_s)
    local.start()

    bar = pltpu.get_barrier_semaphore()
    peers = [me + 1 - 2 * core]
    for s in (SZ, SY, SX):
        for d in STEPS:
            t = shifted(me, s, d)
            peers += [t, t + 1 - 2 * core]
    for t in peers:
        pl.semaphore_signal(bar, inc=1, device_id={'dcp': t}, device_id_type=MESH)
    perms = [onehot((96, 128), lambda r, c, tok=tok: by_set(r, c, 4, 1, tok)) for tok in range(2)]
    queries.wait()
    both = [jnp.dot(perm, qlocal[...].reshape(2 * BATCH, WIDTH), preferred_element_type=F32).astype(BF16) for perm in perms]
    for tok in range(2):
        qsend[:, :, :, pl.ds(tok * LATENT, LATENT)] = both[tok][:, :LATENT].reshape(3, 8, 4, LATENT)
    rotary = jnp.concatenate([both[0][:, LATENT:], both[1][:, LATENT:]], axis=1)
    qsend[:, :, :, pl.ds(2 * LATENT, 2 * ROPE)] = rotary.reshape(3, 8, 4, 2 * ROPE)
    pl.semaphore_wait(bar, len(peers))
    own = [coord(me, RING[k]) * 2 + core for k in range(3)]

    def ring_dest(k, d, flip):
        dev = shifted(me, RING[k], d)
        dcore = core
        if flip:
            dev = dev + 1 - 2 * core
            dcore = 1 - core
        return dev, coord(dev, RING[k]) * 2 + dcore

    near = [(d, flip) for flip in range(2) for d in STEPS[:2]]
    far = [(STEPS[2], flip) for flip in range(2)] + [(0, 1)]
    others = near + far

    for k in range(3):
        for d, flip in others:
            dev, o = ring_dest(k, d, flip)
            remote(qsend.at[k, o], q0buf.at[k, own[k]], q0_s, q0_r, dev).start()
        q0buf[k, own[k]] = qsend[k, own[k]]

    def latent(b):
        return kv_ref.at[b, :, 0, :, first(LATENT)]

    def send_cache(t, which):
        k, i = t % 3, t // 3
        for d, flip in which:
            dev, o = ring_dest(k, d, flip)
            remote(latent(BASE[k] + o * COUNT[k] + i), kvbuf.at[t, own[k]], kv_s, kv_r.at[t], dev).start()
    for t in range(3):
        send_cache(t, near)
    send_cache(2, far)
    big = [coord(me, BIG[k]) for k in range(3)]
    small = [coord(me, SMALL[k]) for k in range(3)]
    arrived(q0buf.at[:, first(7)], q0_r)
    for k in range(3):
        n = COUNT[k]
        order = onehot((n * 8, 32), lambda r, c: c == ((r & 7) << 2) + (r >> 3))
        piece = jnp.dot(order, q0buf[k].reshape(32, QW), preferred_element_type=F32).astype(BF16)
        qbuf[k, first(n), big[k], small[k]] = piece.reshape(n, 8, QW)
    for j, (k, i, n, last_big) in enumerate(UNITS):
        view = qbuf.at[k, pl.ds(i, n), big[k], small[k]]
        for d in STEPS:
            dev = shifted(me, SMALL[k] if last_big else BIG[k], d)
            remote(view, view, q1_s, q1_r.at[j], dev).start()
    for t in range(2):
        send_cache(t, far)

    def block(u, idx, lo, cnt):
        k, i, n, last_big = UNITS[u]
        if last_big:
            return qbuf.at[k, pl.ds(i, n), idx, pl.ds(lo, cnt)]
        return qbuf.at[k, pl.ds(i, n), pl.ds(lo, cnt), idx]

    mid = [big[k] if last_big else small[k] for k, i, n, last_big in UNITS]
    axis = [BIG[k] if last_big else SMALL[k] for k, i, n, last_big in UNITS]
    for u in range(4):
        arrived(block(u, 0, 0, 3), q1_r.at[u])
        view = block(u, mid[u], 0, 4)
        for j, d in enumerate(STEPS[:2]):
            remote(view, view, q2_s, q2_r.at[u, j], shifted(me, axis[u], d)).start()
    local.wait()
    def pack(b, carry):
        ropes[b] = jnp.concatenate([kvlocal[b, 0, :, pl.ds(LATENT, ROPE)], kvlocal[b, 1, :, pl.ds(LATENT, ROPE)]], axis=1)
        return carry

    lax.fori_loop(0, BATCH, pack, 0, unroll=4)
    for k in range(3):
        n = COUNT[k]
        for d, flip in others:
            dev, o = ring_dest(k, d, flip)
            remote(ropes.at[pl.ds(BASE[k] + o * n, n)], kvrope.at[k, own[k], first(n)], kr_s, kr_r, dev).start()
        kvrope[k, own[k], first(n)] = ropes[pl.ds(BASE[k] + own[k] * n, n)]

    send_cache(3, others)
    send_cache(4, others[:2])
    send_cache(5, others[:2])

    def forward(k):
        for j, d in enumerate(STEPS[:2]):
            arrived(block(k, mid[k], 0, 4), q2_r.at[k, j])
            half = block(k, lax.rem(mid[k] + (3 if j == 0 else 1), 4), 2 * j, 2)
            remote(half, half, q3_s, q3_r, shifted(me, axis[k], d)).start()
    forward(2)
    forward(3)
    send_cache(4, others[2:])
    send_cache(6, others)
    send_cache(7, others)
    forward(0)
    forward(1)
    send_cache(5, others[2:])
    for t in range(SLOTS):
        k, i = t % 3, t // 3
        pltpu.make_async_copy(latent(BASE[k] + own[k] * COUNT[k] + i), kvbuf.at[t, own[k]], kv_l).start()

    lens.wait()
    arrived(qbuf.at[first(2), 0], q3_r)
    arrived(ropes.at[first(56)], kr_r)
    arrived(kvbuf.at[:, 0], kv_l)
    def attend(t, carry):
        k = lax.rem(t, 3)
        i = lax.div(t, 3)
        ring = pick(k, RING)
        u = coord(me, ring)
        bstride = pick(k, BIG)
        b_me = coord(me, bstride)
        length = len_ref[24 * k + (u * 2 + core) * pick(k, COUNT) + i]
        arrived(kvbuf.at[t, first(7)], kv_r.at[t])
        q2 = qbuf[k, i].reshape(128, QW)
        q = jnp.concatenate([q2[:, :LATENT], q2[:, LATENT:2 * LATENT]], axis=0)
        pair = q2[:, 2 * LATENT:]
        swapped = jnp.concatenate([pair[:, ROPE:], pair[:, :ROPE]], axis=1)
        low = lax.broadcasted_iota(jnp.int32, pair.shape, 1) < ROPE
        qr = jnp.concatenate([jnp.where(low, pair, swapped), jnp.where(low, swapped, pair)], axis=0)
        keys = kvbuf[t].reshape(1024, LATENT)
        packed = kvrope[k, :, i]
        lane = lax.broadcasted_iota(jnp.int32, packed.shape, 2)
        zero = jnp.zeros_like(packed)
        rope = jnp.stack([jnp.where(lane < ROPE, packed, zero), jnp.where(lane >= ROPE, packed, zero)], axis=1).reshape(1024, 2 * ROPE)
        nt = (((1,), (1,)), ((), ()))
        s = lax.dot_general(q, keys, nt, preferred_element_type=F32)
        s = s + lax.dot_general(qr, rope, nt, preferred_element_type=F32)
        s = s * SCALE
        kk = lax.broadcasted_iota(jnp.int32, (1, 1024), 1)
        dsrc = (me - u * ring - core) + (kk >> 8) * ring + ((kk >> 7) & 1)
        pos = (((kk >> 6) & 1) * GROUP + dsrc) * PAGE + (kk & 63)
        tok = lax.broadcasted_iota(jnp.int32, (256, 1), 0) >> 7
        s = jnp.where(pos - tok <= length - 2, s, MASKED)
        m = jnp.max(s, axis=1, keepdims=True)
        w = jnp.exp(s - m)
        l = jnp.sum(w, axis=1, keepdims=True)
        part = jnp.dot(w.astype(BF16), keys, preferred_element_type=F32)
        part = (part * (1.0 / l)).astype(BF16)
        obuf[k, i, :, :, first(8)] = part[:128].reshape(4, 4, 8, LATENT)
        obuf[k, i, :, :, pl.ds(8, 8)] = part[128:].reshape(4, 4, 8, LATENT)
        lse = m + jnp.log(l)
        l1send[k, i] = tile_lse(jnp.concatenate([lse[:128].reshape(4, 4, 8, 1), lse[128:].reshape(4, 4, 8, 1)], axis=2))
        for d in SENDS:
            b = lax.rem(b_me + d, 4)
            dev = me + (b - b_me) * bstride
            remote(obuf.at[k, i, b], r1buf.at[t, b_me], r1_s, r1_r.at[t], dev).start()
            remote(l1send.at[k, i, b], l1recv.at[t, b_me], l1_s, l1_r.at[t], dev).start()
        r1buf[t, b_me] = obuf[k, i, b_me]
        l1recv[t, b_me] = l1send[k, i, b_me]
        return carry

    lax.fori_loop(0, SLOTS, attend, 0)

    def merge(lse, ref):
        top = jnp.max(lse, axis=0)
        e = jnp.exp(lse - top[None])
        total = jnp.sum(e, axis=0)
        wgt = e / total[None]
        acc = wgt[0] * ref[0].astype(F32)
        for p in range(1, ref.shape[0]):
            acc = acc + wgt[p] * ref[p].astype(F32)
        return acc.astype(BF16), top + jnp.log(total)

    lacc = [jnp.zeros((4, 16, 128), F32) for _ in range(3)]
    for t in (0, 2, 1, 3, 5, 4, 6, 7):
        k, i = t % 3, t // 3
        arrived(l1recv.at[t, first(3)], l1_r.at[t])
        arrived(r1buf.at[t, first(3)], r1_r.at[t])
        both, lse = merge(untile_lse(l1recv[t].astype(F32)), r1buf.at[t])
        m1buf[k, i] = both
        lacc[k] = put_lse(lacc[k], lse, i)
        for d in SENDS:
            b = lax.rem(small[k] + d, 4)
            remote(m1buf.at[k, i, b], r2buf.at[t, small[k]], r2_s, r2_r.at[k], shifted(me, SMALL[k], d)).start()
        r2buf[t, small[k]] = m1buf[k, i, small[k]]
        if i == COUNT[k] - 1:
            l2send[k] = lacc[k].astype(BF16)
            for d in SENDS:
                b = lax.rem(small[k] + d, 4)
                remote(l2send.at[k, b], l2recv.at[k, small[k]], l2_s, l2_r.at[k], shifted(me, SMALL[k], d)).start()
            l2recv[k, small[k]] = l2send[k, small[k]]

    for k in (2, 0, 1):
        n = COUNT[k]
        arrived(l2recv.at[k, first(3)], l2_r.at[k])
        arrived(r2buf.at[first(n), first(3)], r2_r.at[k])
        lr = l2recv[k].astype(F32)
        merged = []
        for i in range(n):
            t = 3 * i + k
            merged.append(merge(get_lse(lr, i), r2buf.at[t])[0])
        order = onehot((64, n * 16), lambda r, c: r == ((c & 7) << 3) + ((c >> 4) << 1) + ((c >> 3) & 1))
        out = jnp.dot(order, jnp.concatenate(merged, axis=0), preferred_element_type=F32)
        fsend[k] = out.astype(BF16).reshape(8, 8, LATENT)
        for d, flip in far + near:
            dev, o = ring_dest(k, d, flip)
            remote(fsend.at[k, o], frecv.at[k, own[k]], f_s, f_r, dev).start()
        frecv[k, own[k]] = fsend[k, own[k]]
    back = onehot((128, 192), lambda r, c: by_set(c, r, 8, 2, 0))
    arrived(frecv.at[:, first(7)], f_r)
    out = jnp.dot(back, frecv[...].reshape(192, LATENT), preferred_element_type=F32)
    out_ref[...] = out.astype(BF16).reshape(BATCH, 2, LATENT)
    def sent(view, sem):
        remote(view, view, sem, sem, me).wait_send()

    sent(q0buf.at[:, first(7)], q0_s)
    sent(qbuf.at[first(2), :, :, 0], q1_s)
    sent(qbuf.at[first(2), first(2)], q2_s)
    sent(qbuf.at[first(2), 0], q3_s)
    sent(ropes.at[first(56)], kr_s)
    sent(kvbuf.at[:, first(7)], kv_s)
    sent(r1buf.at[first(SLOTS), first(3)], r1_s)
    sent(l1recv.at[first(SLOTS), first(3)], l1_s)
    sent(r2buf.at[first(SLOTS), first(3)], r2_s)
    sent(l2recv.at[:, first(3)], l2_s)
    sent(frecv.at[:, first(7)], f_s)


def solution(mesh):
    def local_step(q_blk, kv_blk, len_blk):
        dma = pltpu.SemaphoreType.DMA
        vmem = pltpu.VMEM

        def hbm(v):
            return pltpu.with_memory_space_constraint(v, pltpu.HBM)

        out = pl.pallas_call(
            kernel,
            out_shape=jax.ShapeDtypeStruct((BATCH, 2, LATENT), BF16),
            in_specs=[
                pl.BlockSpec(memory_space=pltpu.HBM),
                pl.BlockSpec(memory_space=pltpu.HBM),
                pl.BlockSpec(memory_space=pltpu.HBM),
            ],
            out_specs=pl.BlockSpec(memory_space=pltpu.VMEM),
            scratch_shapes=[
                pltpu.SMEM((BATCH,), jnp.int32),
                vmem((BATCH, 2, WIDTH), BF16),
                vmem((BATCH, 2, PAGE, WIDTH), BF16),
                vmem((BATCH, PAGE, 2 * ROPE), BF16),
                vmem((SLOTS, 8, 2, PAGE, LATENT), BF16),
                vmem((3, 8, 3, PAGE, 2 * ROPE), BF16),
                vmem((3, 8, 4, QW), BF16),
                vmem((3, 8, 4, QW), BF16),
                vmem((3, 3, 4, 4, 8, QW), BF16),
                vmem((3, 3, 4, 4, 16, LATENT), BF16),
                vmem((SLOTS, 4, 4, 16, LATENT), BF16),
                vmem((3, 3, 4, 16, LATENT), BF16),
                vmem((SLOTS, 4, 16, LATENT), BF16),
                vmem((3, 3, 4, 16, 128), BF16),
                vmem((SLOTS, 4, 16, 128), BF16),
                vmem((3, 4, 16, 128), BF16),
                vmem((3, 4, 16, 128), BF16),
                vmem((3, 8, 8, LATENT), BF16),
                vmem((3, 8, 8, LATENT), BF16),
                dma, dma, dma,
                dma, dma((SLOTS,)), dma,
                dma, dma,
                dma, dma,
                dma, dma((4,)),
                dma, dma((4, 2)),
                dma, dma,
                dma, dma((SLOTS,)),
                dma, dma((3,)),
                dma, dma((SLOTS,)),
                dma, dma((3,)),
                dma, dma,
            ],
            compiler_params=pltpu.CompilerParams(collective_id=0, has_side_effects=True, vmem_limit_bytes=44 * 1024 * 1024),
            name='mla',
        )(hbm(len_blk), hbm(q_blk.reshape(BATCH, 2, WIDTH)), kv_blk)
        return out.reshape(BATCH, 2, 1, LATENT)

    return jax.shard_map(local_step, mesh=mesh, in_specs=(P('dp', None, 'dcp', None), P('dp', None, 'dcp', None, None), P('dp')), out_specs=P('dp', None, 'dcp', None), check_vma=False)
```

```python
import jax
import jax.numpy as jnp
from jax import lax
from jax.experimental import pallas as pl
from jax.experimental.pallas import tpu as pltpu
from jax.sharding import PartitionSpec as P

LATENT = 512
ROPE = 64
NOPE = 128
WIDTH = LATENT + ROPE
QW = 2 * LATENT + 2 * ROPE
PAGE = 64
GROUP = 128
BATCH = 64
MASKED = -1e30
SCALE = (NOPE + ROPE) ** -0.5
MESH = pl.DeviceIdType.MESH
BF16 = jnp.bfloat16
F32 = jnp.float32

SZ, SY, SX = 32, 8, 2
RING = (SZ, SY, SX)
BIG = (SX, SZ, SY)
SMALL = (SY, SX, SZ)
COUNT = (3, 3, 2)
BASE = (0, 24, 48)
SLOTS = 8
STEPS = (1, 3, 2)
SENDS = (2, 1, 3)
UNITS = ((0, 0, 3, True), (1, 0, 3, False), (2, 0, 2, True))


def pick(k, vals):
    return jnp.where(k == 0, vals[0], jnp.where(k == 1, vals[1], vals[2]))


def coord(me, stride):
    return lax.rem(lax.div(me, stride), 4)


def shifted(me, stride, d):
    c = coord(me, stride)
    return me + (lax.rem(c + d, 4) - c) * stride


def remote(src, dst, ssem, rsem, dev):
    return pltpu.make_async_remote_copy(src_ref=src, dst_ref=dst, send_sem=ssem, recv_sem=rsem, device_id={'dcp': dev}, device_id_type=MESH)


def arrived(view, sem):
    pltpu.make_async_copy(view, view, sem).wait()


def split3(v):
    hi = v.astype(BF16).astype(F32)
    mid = (v - hi).astype(BF16).astype(F32)
    return hi, mid, v - hi - mid


def put_lse(tile, lse, b):
    lane = lax.broadcasted_iota(jnp.int32, tile.shape, len(tile.shape) - 1)
    for j, v in enumerate(split3(lse)):
        tile = jnp.where(lane == 32 * b + j, v, tile)
    return tile


def get_lse(x, b):
    return sum(x[..., 32 * b + j:32 * b + j + 1] for j in range(3))


def tile_lse(lse):
    tile = jnp.zeros((4, 16, 128), F32)
    for b in range(4):
        tile = put_lse(tile, lse[:, b], b)
    return tile.astype(BF16)


def untile_lse(x):
    return jnp.stack([get_lse(x, b) for b in range(4)], axis=1)


def first(count):
    return pl.ds(0, count)


def onehot(shape, fn):
    row = lax.broadcasted_iota(jnp.int32, shape, 0)
    col = lax.broadcasted_iota(jnp.int32, shape, 1)
    return jnp.where(fn(row, col), 1.0, 0.0).astype(BF16)


def by_set(rows, cols, pad, tokens, tok):
    hit = None
    for k in range(3):
        n = COUNT[k]
        r = rows - k * 8 * pad
        o, j = lax.div(jnp.maximum(r, 0), pad), r & (pad - 1)
        m = (r >= 0) & (r < 8 * pad) & (j < n * tokens) & (cols == 2 * (BASE[k] + o * n) + (2 // tokens) * j + tok)
        hit = m if hit is None else hit | m
    return hit


def kernel(len_hbm, q_ref, kv_ref, out_ref, len_ref, qlocal, kvlocal, ropes, kvbuf, kvrope, qsend, q0buf, qbuf, obuf, r1buf, m1buf, r2buf,
           l1send, l1recv, l2send, l2recv, fsend, frecv,
           len_s, ql_s, loc_s, kv_s, kv_r, kv_l, kr_s, kr_r, q0_s, q0_r, q1_s, q1_r, q2_s, q2_r, q3_s, q3_r, r1_s, r1_r, r2_s, r2_r,
           l1_s, l1_r, l2_s, l2_r, f_s, f_r):
    me = lax.axis_index('dcp')
    core = lax.rem(me, 2)
    queries = pltpu.make_async_copy(q_ref, qlocal, ql_s)
    queries.start()
    lens = pltpu.make_async_copy(len_hbm, len_ref, len_s)
    lens.start()
    local = pltpu.make_async_copy(kv_ref.at[:, :, 0], kvlocal, loc_s)
    local.start()

    bar = pltpu.get_barrier_semaphore()
    peers = [me + 1 - 2 * core]
    for s in (SZ, SY, SX):
        for d in STEPS:
            t = shifted(me, s, d)
            peers += [t, t + 1 - 2 * core]
    for t in peers:
        pl.semaphore_signal(bar, inc=1, device_id={'dcp': t}, device_id_type=MESH)
    perms = [onehot((96, 128), lambda r, c, tok=tok: by_set(r, c, 4, 1, tok)) for tok in range(2)]
    queries.wait()
    both = [jnp.dot(perm, qlocal[...].reshape(2 * BATCH, WIDTH), preferred_element_type=F32).astype(BF16) for perm in perms]
    for tok in range(2):
        qsend[:, :, :, pl.ds(tok * LATENT, LATENT)] = both[tok][:, :LATENT].reshape(3, 8, 4, LATENT)
    rotary = jnp.concatenate([both[0][:, LATENT:], both[1][:, LATENT:]], axis=1)
    qsend[:, :, :, pl.ds(2 * LATENT, 2 * ROPE)] = rotary.reshape(3, 8, 4, 2 * ROPE)
    pl.semaphore_wait(bar, len(peers))
    own = [coord(me, RING[k]) * 2 + core for k in range(3)]

    def ring_dest(k, d, flip):
        dev = shifted(me, RING[k], d)
        dcore = core
        if flip:
            dev = dev + 1 - 2 * core
            dcore = 1 - core
        return dev, coord(dev, RING[k]) * 2 + dcore

    near = [(d, flip) for flip in range(2) for d in STEPS[:2]]
    far = [(STEPS[2], flip) for flip in range(2)] + [(0, 1)]
    others = near + far

    for k in range(3):
        for d, flip in others:
            dev, o = ring_dest(k, d, flip)
            remote(qsend.at[k, o], q0buf.at[k, own[k]], q0_s, q0_r, dev).start()
        q0buf[k, own[k]] = qsend[k, own[k]]

    def latent(b):
        return kv_ref.at[b, :, 0, :, first(LATENT)]

    def send_cache(t, which):
        k, i = t % 3, t // 3
        for d, flip in which:
            dev, o = ring_dest(k, d, flip)
            remote(latent(BASE[k] + o * COUNT[k] + i), kvbuf.at[t, own[k]], kv_s, kv_r.at[t], dev).start()
    for t in range(3):
        send_cache(t, near)
    send_cache(2, far)
    big = [coord(me, BIG[k]) for k in range(3)]
    small = [coord(me, SMALL[k]) for k in range(3)]
    arrived(q0buf.at[:, first(7)], q0_r)
    for k in range(3):
        n = COUNT[k]
        order = onehot((n * 8, 32), lambda r, c: c == ((r & 7) << 2) + (r >> 3))
        piece = jnp.dot(order, q0buf[k].reshape(32, QW), preferred_element_type=F32).astype(BF16)
        qbuf[k, first(n), big[k], small[k]] = piece.reshape(n, 8, QW)
    for j, (k, i, n, last_big) in enumerate(UNITS):
        view = qbuf.at[k, pl.ds(i, n), big[k], small[k]]
        for d in STEPS:
            dev = shifted(me, SMALL[k] if last_big else BIG[k], d)
            remote(view, view, q1_s, q1_r.at[j], dev).start()
    for t in range(2):
        send_cache(t, far)

    def block(u, idx, lo, cnt):
        k, i, n, last_big = UNITS[u]
        if last_big:
            return qbuf.at[k, pl.ds(i, n), idx, pl.ds(lo, cnt)]
        return qbuf.at[k, pl.ds(i, n), pl.ds(lo, cnt), idx]

    mid = [big[k] if last_big else small[k] for k, i, n, last_big in UNITS]
    axis = [BIG[k] if last_big else SMALL[k] for k, i, n, last_big in UNITS]
    for u in range(3):
        arrived(block(u, 0, 0, 3), q1_r.at[u])
        view = block(u, mid[u], 0, 4)
        for j, d in enumerate(STEPS[:2]):
            remote(view, view, q2_s, q2_r.at[u, j], shifted(me, axis[u], d)).start()
    local.wait()
    def pack(b, carry):
        ropes[b] = jnp.concatenate([kvlocal[b, 0, :, pl.ds(LATENT, ROPE)], kvlocal[b, 1, :, pl.ds(LATENT, ROPE)]], axis=1)
        return carry

    lax.fori_loop(0, BATCH, pack, 0, unroll=4)
    for k in range(3):
        n = COUNT[k]
        for d, flip in others:
            dev, o = ring_dest(k, d, flip)
            remote(ropes.at[pl.ds(BASE[k] + o * n, n)], kvrope.at[k, own[k], first(n)], kr_s, kr_r, dev).start()
        kvrope[k, own[k], first(n)] = ropes[pl.ds(BASE[k] + own[k] * n, n)]

    send_cache(3, others)
    send_cache(4, others[:2])
    send_cache(5, others[:2])

    def forward(k):
        for j, d in enumerate(STEPS[:2]):
            arrived(block(k, mid[k], 0, 4), q2_r.at[k, j])
            half = block(k, lax.rem(mid[k] + (3 if j == 0 else 1), 4), 2 * j, 2)
            remote(half, half, q3_s, q3_r.at[k], shifted(me, axis[k], d)).start()
    forward(2)
    send_cache(4, others[2:])
    send_cache(6, others)
    send_cache(7, others)
    forward(0)
    forward(1)
    send_cache(5, others[2:])
    for t in range(SLOTS):
        k, i = t % 3, t // 3
        pltpu.make_async_copy(latent(BASE[k] + own[k] * COUNT[k] + i), kvbuf.at[t, own[k]], kv_l).start()

    lens.wait()
    arrived(ropes.at[first(56)], kr_r)
    arrived(kvbuf.at[:, 0], kv_l)
    def attend(t, carry):
        k = lax.rem(t, 3)
        i = lax.div(t, 3)
        ring = pick(k, RING)
        u = coord(me, ring)
        bstride = pick(k, BIG)
        b_me = coord(me, bstride)
        length = len_ref[24 * k + (u * 2 + core) * pick(k, COUNT) + i]
        for unit in range(3):

            @pl.when(t == unit)
            def _():
                arrived(block(unit, 0, 0, 4), q3_r.at[unit])
        arrived(kvbuf.at[t, first(7)], kv_r.at[t])
        q2 = qbuf[k, i].reshape(128, QW)
        q = jnp.concatenate([q2[:, :LATENT], q2[:, LATENT:2 * LATENT]], axis=0)
        pair = q2[:, 2 * LATENT:]
        swapped = jnp.concatenate([pair[:, ROPE:], pair[:, :ROPE]], axis=1)
        low = lax.broadcasted_iota(jnp.int32, pair.shape, 1) < ROPE
        qr = jnp.concatenate([jnp.where(low, pair, swapped), jnp.where(low, swapped, pair)], axis=0)
        keys = kvbuf[t].reshape(1024, LATENT)
        packed = kvrope[k, :, i]
        lane = lax.broadcasted_iota(jnp.int32, packed.shape, 2)
        zero = jnp.zeros_like(packed)
        rope = jnp.stack([jnp.where(lane < ROPE, packed, zero), jnp.where(lane >= ROPE, packed, zero)], axis=1).reshape(1024, 2 * ROPE)
        nt = (((1,), (1,)), ((), ()))
        s = lax.dot_general(q, keys, nt, preferred_element_type=F32)
        s = s + lax.dot_general(qr, rope, nt, preferred_element_type=F32)
        s = s * SCALE
        kk = lax.broadcasted_iota(jnp.int32, (1, 1024), 1)
        dsrc = (me - u * ring - core) + (kk >> 8) * ring + ((kk >> 7) & 1)
        pos = (((kk >> 6) & 1) * GROUP + dsrc) * PAGE + (kk & 63)
        tok = lax.broadcasted_iota(jnp.int32, (256, 1), 0) >> 7
        s = jnp.where(pos - tok <= length - 2, s, MASKED)
        m = jnp.max(s, axis=1, keepdims=True)
        w = jnp.exp(s - m)
        l = jnp.sum(w, axis=1, keepdims=True)
        part = jnp.dot(w.astype(BF16), keys, preferred_element_type=F32)
        part = (part * (1.0 / l)).astype(BF16)
        obuf[k, i, :, :, first(8)] = part[:128].reshape(4, 4, 8, LATENT)
        obuf[k, i, :, :, pl.ds(8, 8)] = part[128:].reshape(4, 4, 8, LATENT)
        lse = m + jnp.log(l)
        l1send[k, i] = tile_lse(jnp.concatenate([lse[:128].reshape(4, 4, 8, 1), lse[128:].reshape(4, 4, 8, 1)], axis=2))
        for d in SENDS:
            b = lax.rem(b_me + d, 4)
            dev = me + (b - b_me) * bstride
            remote(obuf.at[k, i, b], r1buf.at[t, b_me], r1_s, r1_r.at[t], dev).start()
            remote(l1send.at[k, i, b], l1recv.at[t, b_me], l1_s, l1_r.at[t], dev).start()
        r1buf[t, b_me] = obuf[k, i, b_me]
        l1recv[t, b_me] = l1send[k, i, b_me]
        return carry

    lax.fori_loop(0, SLOTS, attend, 0)

    def merge(lse, ref):
        top = jnp.max(lse, axis=0)
        e = jnp.exp(lse - top[None])
        total = jnp.sum(e, axis=0)
        wgt = e / total[None]
        acc = wgt[0] * ref[0].astype(F32)
        for p in range(1, ref.shape[0]):
            acc = acc + wgt[p] * ref[p].astype(F32)
        return acc.astype(BF16), top + jnp.log(total)

    lacc = [jnp.zeros((4, 16, 128), F32) for _ in range(3)]
    for t in (0, 2, 1, 3, 5, 4, 6, 7):
        k, i = t % 3, t // 3
        arrived(l1recv.at[t, first(3)], l1_r.at[t])
        arrived(r1buf.at[t, first(3)], r1_r.at[t])
        both, lse = merge(untile_lse(l1recv[t].astype(F32)), r1buf.at[t])
        m1buf[k, i] = both
        lacc[k] = put_lse(lacc[k], lse, i)
        for d in SENDS:
            b = lax.rem(small[k] + d, 4)
            remote(m1buf.at[k, i, b], r2buf.at[t, small[k]], r2_s, r2_r.at[k], shifted(me, SMALL[k], d)).start()
        r2buf[t, small[k]] = m1buf[k, i, small[k]]
        if i == COUNT[k] - 1:
            l2send[k] = lacc[k].astype(BF16)
            for d in SENDS:
                b = lax.rem(small[k] + d, 4)
                remote(l2send.at[k, b], l2recv.at[k, small[k]], l2_s, l2_r.at[k], shifted(me, SMALL[k], d)).start()
            l2recv[k, small[k]] = l2send[k, small[k]]

    for k in (2, 0, 1):
        n = COUNT[k]
        arrived(l2recv.at[k, first(3)], l2_r.at[k])
        arrived(r2buf.at[first(n), first(3)], r2_r.at[k])
        lr = l2recv[k].astype(F32)
        merged = []
        for i in range(n):
            t = 3 * i + k
            merged.append(merge(get_lse(lr, i), r2buf.at[t])[0])
        order = onehot((64, n * 16), lambda r, c: r == ((c & 7) << 3) + ((c >> 4) << 1) + ((c >> 3) & 1))
        out = jnp.dot(order, jnp.concatenate(merged, axis=0), preferred_element_type=F32)
        fsend[k] = out.astype(BF16).reshape(8, 8, LATENT)
        for d, flip in far + near:
            dev, o = ring_dest(k, d, flip)
            remote(fsend.at[k, o], frecv.at[k, own[k]], f_s, f_r, dev).start()
        frecv[k, own[k]] = fsend[k, own[k]]
    back = onehot((128, 192), lambda r, c: by_set(c, r, 8, 2, 0))
    arrived(frecv.at[:, first(7)], f_r)
    out = jnp.dot(back, frecv[...].reshape(192, LATENT), preferred_element_type=F32)
    out_ref[...] = out.astype(BF16).reshape(BATCH, 2, LATENT)
    def sent(view, sem):
        remote(view, view, sem, sem, me).wait_send()

    sent(q0buf.at[:, first(7)], q0_s)
    sent(qbuf.at[first(2), :, :, 0], q1_s)
    sent(qbuf.at[first(2), first(2)], q2_s)
    sent(qbuf.at[first(2), 0], q3_s)
    sent(ropes.at[first(56)], kr_s)
    sent(kvbuf.at[:, first(7)], kv_s)
    sent(r1buf.at[first(SLOTS), first(3)], r1_s)
    sent(l1recv.at[first(SLOTS), first(3)], l1_s)
    sent(r2buf.at[first(SLOTS), first(3)], r2_s)
    sent(l2recv.at[:, first(3)], l2_s)
    sent(frecv.at[:, first(7)], f_s)


def solution(mesh):
    def local_step(q_blk, kv_blk, len_blk):
        dma = pltpu.SemaphoreType.DMA
        vmem = pltpu.VMEM

        def hbm(v):
            return pltpu.with_memory_space_constraint(v, pltpu.HBM)

        out = pl.pallas_call(
            kernel,
            out_shape=jax.ShapeDtypeStruct((BATCH, 2, LATENT), BF16),
            in_specs=[
                pl.BlockSpec(memory_space=pltpu.HBM),
                pl.BlockSpec(memory_space=pltpu.HBM),
                pl.BlockSpec(memory_space=pltpu.HBM),
            ],
            out_specs=pl.BlockSpec(memory_space=pltpu.VMEM),
            scratch_shapes=[
                pltpu.SMEM((BATCH,), jnp.int32),
                vmem((BATCH, 2, WIDTH), BF16),
                vmem((BATCH, 2, PAGE, WIDTH), BF16),
                vmem((BATCH, PAGE, 2 * ROPE), BF16),
                vmem((SLOTS, 8, 2, PAGE, LATENT), BF16),
                vmem((3, 8, 3, PAGE, 2 * ROPE), BF16),
                vmem((3, 8, 4, QW), BF16),
                vmem((3, 8, 4, QW), BF16),
                vmem((3, 3, 4, 4, 8, QW), BF16),
                vmem((3, 3, 4, 4, 16, LATENT), BF16),
                vmem((SLOTS, 4, 4, 16, LATENT), BF16),
                vmem((3, 3, 4, 16, LATENT), BF16),
                vmem((SLOTS, 4, 16, LATENT), BF16),
                vmem((3, 3, 4, 16, 128), BF16),
                vmem((SLOTS, 4, 16, 128), BF16),
                vmem((3, 4, 16, 128), BF16),
                vmem((3, 4, 16, 128), BF16),
                vmem((3, 8, 8, LATENT), BF16),
                vmem((3, 8, 8, LATENT), BF16),
                dma, dma, dma,
                dma, dma((SLOTS,)), dma,
                dma, dma,
                dma, dma,
                dma, dma((3,)),
                dma, dma((3, 2)),
                dma, dma((3,)),
                dma, dma((SLOTS,)),
                dma, dma((3,)),
                dma, dma((SLOTS,)),
                dma, dma((3,)),
                dma, dma,
            ],
            compiler_params=pltpu.CompilerParams(collective_id=0, has_side_effects=True, vmem_limit_bytes=44 * 1024 * 1024),
            name='mla',
        )(hbm(len_blk), hbm(q_blk.reshape(BATCH, 2, WIDTH)), kv_blk)
        return out.reshape(BATCH, 2, 1, LATENT)

    return jax.shard_map(local_step, mesh=mesh, in_specs=(P('dp', None, 'dcp', None), P('dp', None, 'dcp', None, None), P('dp')), out_specs=P('dp', None, 'dcp', None), check_vma=False)
```

```python
import jax
import jax.numpy as jnp
from jax import lax
from jax.experimental import pallas as pl
from jax.experimental.pallas import tpu as pltpu
from jax.sharding import PartitionSpec as P

LATENT = 512
ROPE = 64
NOPE = 128
WIDTH = LATENT + ROPE
QW = 2 * LATENT + 2 * ROPE
PAGE = 64
GROUP = 128
BATCH = 64
MASKED = -1e30
SCALE = (NOPE + ROPE) ** -0.5
MESH = pl.DeviceIdType.MESH
BF16 = jnp.bfloat16
F32 = jnp.float32

SZ, SY, SX = 32, 8, 2
RING = (SZ, SY, SX)
BIG = (SX, SZ, SY)
SMALL = (SY, SX, SZ)
COUNT = (3, 3, 2)
BASE = (0, 24, 48)
SLOTS = 8
STEPS = (1, 3, 2)
SENDS = (2, 1, 3)
UNITS = ((0, 0, 3, True), (1, 0, 3, False), (2, 0, 2, True))


def pick(k, vals):
    return jnp.where(k == 0, vals[0], jnp.where(k == 1, vals[1], vals[2]))


def coord(me, stride):
    return lax.rem(lax.div(me, stride), 4)


def shifted(me, stride, d):
    c = coord(me, stride)
    return me + (lax.rem(c + d, 4) - c) * stride


def remote(src, dst, ssem, rsem, dev):
    return pltpu.make_async_remote_copy(src_ref=src, dst_ref=dst, send_sem=ssem, recv_sem=rsem, device_id={'dcp': dev}, device_id_type=MESH)


def arrived(view, sem):
    pltpu.make_async_copy(view, view, sem).wait()


def split3(v):
    hi = v.astype(BF16).astype(F32)
    mid = (v - hi).astype(BF16).astype(F32)
    return hi, mid, v - hi - mid


def put_lse(tile, lse, b):
    lane = lax.broadcasted_iota(jnp.int32, tile.shape, len(tile.shape) - 1)
    for j, v in enumerate(split3(lse)):
        tile = jnp.where(lane == 32 * b + j, v, tile)
    return tile


def get_lse(x, b):
    return sum(x[..., 32 * b + j:32 * b + j + 1] for j in range(3))


def tile_lse(lse):
    tile = jnp.zeros((4, 16, 128), F32)
    for b in range(4):
        tile = put_lse(tile, lse[:, b], b)
    return tile.astype(BF16)


def untile_lse(x):
    return jnp.stack([get_lse(x, b) for b in range(4)], axis=1)


def first(count):
    return pl.ds(0, count)


def onehot(shape, fn):
    row = lax.broadcasted_iota(jnp.int32, shape, 0)
    col = lax.broadcasted_iota(jnp.int32, shape, 1)
    return jnp.where(fn(row, col), 1.0, 0.0).astype(BF16)


def by_set(rows, cols, pad, tokens, tok):
    hit = None
    for k in range(3):
        n = COUNT[k]
        r = rows - k * 8 * pad
        o, j = lax.div(jnp.maximum(r, 0), pad), r & (pad - 1)
        m = (r >= 0) & (r < 8 * pad) & (j < n * tokens) & (cols == 2 * (BASE[k] + o * n) + (2 // tokens) * j + tok)
        hit = m if hit is None else hit | m
    return hit


def kernel(len_hbm, q_ref, kv_ref, out_ref, len_ref, qlocal, kvlocal, ropes, kvbuf, kvrope, qsend, q0buf, qbuf, obuf, r1buf, m1buf, r2buf,
           l1send, l1recv, l2send, l2recv, tally, fsend, frecv,
           len_s, ql_s, loc_s, kv_s, kv_r, kv_l, kr_s, kr_r, q0_s, q0_r, q1_s, q1_r, q2_s, q2_r, q3_s, q3_r, r1_s, r1_r, r2_s, r2_r,
           l1_s, l2_s, f_s, f_r):
    me = lax.axis_index('dcp')
    core = lax.rem(me, 2)
    queries = pltpu.make_async_copy(q_ref, qlocal, ql_s)
    queries.start()
    lens = pltpu.make_async_copy(len_hbm, len_ref, len_s)
    lens.start()
    local = pltpu.make_async_copy(kv_ref.at[:, :, 0], kvlocal, loc_s)
    local.start()

    bar = pltpu.get_barrier_semaphore()
    peers = [me + 1 - 2 * core]
    for s in (SZ, SY, SX):
        for d in STEPS:
            t = shifted(me, s, d)
            peers += [t, t + 1 - 2 * core]
    for t in peers:
        pl.semaphore_signal(bar, inc=1, device_id={'dcp': t}, device_id_type=MESH)
    perms = [onehot((96, 128), lambda r, c, tok=tok: by_set(r, c, 4, 1, tok)) for tok in range(2)]
    queries.wait()
    both = [jnp.dot(perm, qlocal[...].reshape(2 * BATCH, WIDTH), preferred_element_type=F32).astype(BF16) for perm in perms]
    for tok in range(2):
        qsend[:, :, :, pl.ds(tok * LATENT, LATENT)] = both[tok][:, :LATENT].reshape(3, 8, 4, LATENT)
    rotary = jnp.concatenate([both[0][:, LATENT:], both[1][:, LATENT:]], axis=1)
    qsend[:, :, :, pl.ds(2 * LATENT, 2 * ROPE)] = rotary.reshape(3, 8, 4, 2 * ROPE)
    pl.semaphore_wait(bar, len(peers))
    own = [coord(me, RING[k]) * 2 + core for k in range(3)]

    def ring_dest(k, d, flip):
        dev = shifted(me, RING[k], d)
        dcore = core
        if flip:
            dev = dev + 1 - 2 * core
            dcore = 1 - core
        return dev, coord(dev, RING[k]) * 2 + dcore

    near = [(d, flip) for flip in range(2) for d in STEPS[:2]]
    far = [(STEPS[2], flip) for flip in range(2)] + [(0, 1)]
    others = near + far

    for k in range(3):
        for d, flip in others:
            dev, o = ring_dest(k, d, flip)
            remote(qsend.at[k, o], q0buf.at[k, own[k]], q0_s, q0_r, dev).start()
        q0buf[k, own[k]] = qsend[k, own[k]]

    def latent(b):
        return kv_ref.at[b, :, 0, :, first(LATENT)]

    def send_cache(t, which):
        k, i = t % 3, t // 3
        for d, flip in which:
            dev, o = ring_dest(k, d, flip)
            remote(latent(BASE[k] + o * COUNT[k] + i), kvbuf.at[t, own[k]], kv_s, kv_r.at[t], dev).start()
    for t in range(3):
        send_cache(t, near)
    send_cache(2, far)
    big = [coord(me, BIG[k]) for k in range(3)]
    small = [coord(me, SMALL[k]) for k in range(3)]
    arrived(q0buf.at[:, first(7)], q0_r)
    for k in range(3):
        n = COUNT[k]
        order = onehot((n * 8, 32), lambda r, c: c == ((r & 7) << 2) + (r >> 3))
        piece = jnp.dot(order, q0buf[k].reshape(32, QW), preferred_element_type=F32).astype(BF16)
        qbuf[k, first(n), big[k], small[k]] = piece.reshape(n, 8, QW)
    for j, (k, i, n, last_big) in enumerate(UNITS):
        view = qbuf.at[k, pl.ds(i, n), big[k], small[k]]
        for d in STEPS:
            dev = shifted(me, SMALL[k] if last_big else BIG[k], d)
            remote(view, view, q1_s, q1_r.at[j], dev).start()
    for t in range(2):
        send_cache(t, far)

    def block(u, idx, lo, cnt):
        k, i, n, last_big = UNITS[u]
        if last_big:
            return qbuf.at[k, pl.ds(i, n), idx, pl.ds(lo, cnt)]
        return qbuf.at[k, pl.ds(i, n), pl.ds(lo, cnt), idx]

    mid = [big[k] if last_big else small[k] for k, i, n, last_big in UNITS]
    axis = [BIG[k] if last_big else SMALL[k] for k, i, n, last_big in UNITS]
    for u in range(3):
        arrived(block(u, 0, 0, 3), q1_r.at[u])
        view = block(u, mid[u], 0, 4)
        for j, d in enumerate(STEPS[:2]):
            remote(view, view, q2_s, q2_r.at[u, j], shifted(me, axis[u], d)).start()
    local.wait()
    def pack(b, carry):
        ropes[b] = jnp.concatenate([kvlocal[b, 0, :, pl.ds(LATENT, ROPE)], kvlocal[b, 1, :, pl.ds(LATENT, ROPE)]], axis=1)
        return carry

    lax.fori_loop(0, BATCH, pack, 0, unroll=4)
    for k in range(3):
        n = COUNT[k]
        for d, flip in others:
            dev, o = ring_dest(k, d, flip)
            remote(ropes.at[pl.ds(BASE[k] + o * n, n)], kvrope.at[k, own[k], first(n)], kr_s, kr_r, dev).start()
        kvrope[k, own[k], first(n)] = ropes[pl.ds(BASE[k] + own[k] * n, n)]

    send_cache(3, others)
    send_cache(4, others[:2])
    send_cache(5, others[:2])

    def forward(k):
        for j, d in enumerate(STEPS[:2]):
            arrived(block(k, mid[k], 0, 4), q2_r.at[k, j])
            half = block(k, lax.rem(mid[k] + (3 if j == 0 else 1), 4), 2 * j, 2)
            remote(half, half, q3_s, q3_r.at[k], shifted(me, axis[k], d)).start()
    forward(2)
    send_cache(4, others[2:])
    send_cache(6, others)
    send_cache(7, others)
    forward(0)
    forward(1)
    send_cache(5, others[2:])
    for t in range(SLOTS):
        k, i = t % 3, t // 3
        pltpu.make_async_copy(latent(BASE[k] + own[k] * COUNT[k] + i), kvbuf.at[t, own[k]], kv_l).start()

    lens.wait()
    arrived(ropes.at[first(56)], kr_r)
    arrived(kvbuf.at[:, 0], kv_l)
    def attend(t, carry):
        k = lax.rem(t, 3)
        i = lax.div(t, 3)
        ring = pick(k, RING)
        u = coord(me, ring)
        bstride = pick(k, BIG)
        b_me = coord(me, bstride)
        length = len_ref[24 * k + (u * 2 + core) * pick(k, COUNT) + i]
        for unit in range(3):

            @pl.when(t == unit)
            def _():
                arrived(block(unit, 0, 0, 4), q3_r.at[unit])
        arrived(kvbuf.at[t, first(7)], kv_r.at[t])
        q2 = qbuf[k, i].reshape(128, QW)
        q = jnp.concatenate([q2[:, :LATENT], q2[:, LATENT:2 * LATENT]], axis=0)
        pair = q2[:, 2 * LATENT:]
        swapped = jnp.concatenate([pair[:, ROPE:], pair[:, :ROPE]], axis=1)
        low = lax.broadcasted_iota(jnp.int32, pair.shape, 1) < ROPE
        qr = jnp.concatenate([jnp.where(low, pair, swapped), jnp.where(low, swapped, pair)], axis=0)
        keys = kvbuf[t].reshape(1024, LATENT)
        packed = kvrope[k, :, i]
        lane = lax.broadcasted_iota(jnp.int32, packed.shape, 2)
        zero = jnp.zeros_like(packed)
        rope = jnp.stack([jnp.where(lane < ROPE, packed, zero), jnp.where(lane >= ROPE, packed, zero)], axis=1).reshape(1024, 2 * ROPE)
        nt = (((1,), (1,)), ((), ()))
        s = lax.dot_general(q, keys, nt, preferred_element_type=F32)
        s = s + lax.dot_general(qr, rope, nt, preferred_element_type=F32)
        s = s * SCALE
        kk = lax.broadcasted_iota(jnp.int32, (1, 1024), 1)
        dsrc = (me - u * ring - core) + (kk >> 8) * ring + ((kk >> 7) & 1)
        pos = (((kk >> 6) & 1) * GROUP + dsrc) * PAGE + (kk & 63)
        tok = lax.broadcasted_iota(jnp.int32, (256, 1), 0) >> 7
        s = jnp.where(pos - tok <= length - 2, s, MASKED)
        m = jnp.max(s, axis=1, keepdims=True)
        w = jnp.exp(s - m)
        l = jnp.sum(w, axis=1, keepdims=True)
        part = jnp.dot(w.astype(BF16), keys, preferred_element_type=F32)
        part = (part * (1.0 / l)).astype(BF16)
        obuf[k, i, :, :, first(8)] = part[:128].reshape(4, 4, 8, LATENT)
        obuf[k, i, :, :, pl.ds(8, 8)] = part[128:].reshape(4, 4, 8, LATENT)
        lse = m + jnp.log(l)
        l1send[k, i] = tile_lse(jnp.concatenate([lse[:128].reshape(4, 4, 8, 1), lse[128:].reshape(4, 4, 8, 1)], axis=2))
        for d in SENDS:
            b = lax.rem(b_me + d, 4)
            dev = me + (b - b_me) * bstride
            remote(obuf.at[k, i, b], r1buf.at[t, b_me], r1_s, r1_r.at[t], dev).start()
            remote(l1send.at[k, i, b], l1recv.at[t, b_me], l1_s, r1_r.at[t], dev).start()
        r1buf[t, b_me] = obuf[k, i, b_me]
        l1recv[t, b_me] = l1send[k, i, b_me]
        return carry

    lax.fori_loop(0, SLOTS, attend, 0)

    def merge(lse, ref):
        top = jnp.max(lse, axis=0)
        e = jnp.exp(lse - top[None])
        total = jnp.sum(e, axis=0)
        wgt = e / total[None]
        acc = wgt[0] * ref[0].astype(F32)
        for p in range(1, ref.shape[0]):
            acc = acc + wgt[p] * ref[p].astype(F32)
        return acc.astype(BF16), top + jnp.log(total)

    lacc = [jnp.zeros((4, 16, 128), F32) for _ in range(3)]
    for t in (0, 1, 3, 4, 2, 6, 5, 7):
        k, i = t % 3, t // 3
        arrived(tally.at[first(51)], r1_r.at[t])
        both, lse = merge(untile_lse(l1recv[t].astype(F32)), r1buf.at[t])
        m1buf[k, i] = both
        lacc[k] = put_lse(lacc[k], lse, i)
        for d in SENDS:
            b = lax.rem(small[k] + d, 4)
            remote(m1buf.at[k, i, b], r2buf.at[t, small[k]], r2_s, r2_r.at[k], shifted(me, SMALL[k], d)).start()
        r2buf[t, small[k]] = m1buf[k, i, small[k]]
        if i == COUNT[k] - 1:
            l2send[k] = lacc[k].astype(BF16)
            for d in SENDS:
                b = lax.rem(small[k] + d, 4)
                remote(l2send.at[k, b], l2recv.at[k, small[k]], l2_s, r2_r.at[k], shifted(me, SMALL[k], d)).start()
            l2recv[k, small[k]] = l2send[k, small[k]]

    for k in (0, 2, 1):
        n = COUNT[k]
        arrived(tally.at[first(12 * n + 3)], r2_r.at[k])
        lr = l2recv[k].astype(F32)
        merged = []
        for i in range(n):
            t = 3 * i + k
            merged.append(merge(get_lse(lr, i), r2buf.at[t])[0])
        order = onehot((64, n * 16), lambda r, c: r == ((c & 7) << 3) + ((c >> 4) << 1) + ((c >> 3) & 1))
        out = jnp.dot(order, jnp.concatenate(merged, axis=0), preferred_element_type=F32)
        fsend[k] = out.astype(BF16).reshape(8, 8, LATENT)
        for d, flip in far + near:
            dev, o = ring_dest(k, d, flip)
            remote(fsend.at[k, o], frecv.at[k, own[k]], f_s, f_r, dev).start()
        frecv[k, own[k]] = fsend[k, own[k]]
    back = onehot((128, 192), lambda r, c: by_set(c, r, 8, 2, 0))
    arrived(frecv.at[:, first(7)], f_r)
    out = jnp.dot(back, frecv[...].reshape(192, LATENT), preferred_element_type=F32)
    out_ref[...] = out.astype(BF16).reshape(BATCH, 2, LATENT)
    def sent(view, sem):
        remote(view, view, sem, sem, me).wait_send()

    sent(q0buf.at[:, first(7)], q0_s)
    sent(qbuf.at[first(2), :, :, 0], q1_s)
    sent(qbuf.at[first(2), first(2)], q2_s)
    sent(qbuf.at[first(2), 0], q3_s)
    sent(ropes.at[first(56)], kr_s)
    sent(kvbuf.at[:, first(7)], kv_s)
    sent(r1buf.at[first(SLOTS), first(3)], r1_s)
    sent(l1recv.at[first(SLOTS), first(3)], l1_s)
    sent(r2buf.at[first(SLOTS), first(3)], r2_s)
    sent(l2recv.at[:, first(3)], l2_s)
    sent(frecv.at[:, first(7)], f_s)


def solution(mesh):
    def local_step(q_blk, kv_blk, len_blk):
        dma = pltpu.SemaphoreType.DMA
        vmem = pltpu.VMEM

        def hbm(v):
            return pltpu.with_memory_space_constraint(v, pltpu.HBM)

        out = pl.pallas_call(
            kernel,
            out_shape=jax.ShapeDtypeStruct((BATCH, 2, LATENT), BF16),
            in_specs=[
                pl.BlockSpec(memory_space=pltpu.HBM),
                pl.BlockSpec(memory_space=pltpu.HBM),
                pl.BlockSpec(memory_space=pltpu.HBM),
            ],
            out_specs=pl.BlockSpec(memory_space=pltpu.VMEM),
            scratch_shapes=[
                pltpu.SMEM((BATCH,), jnp.int32),
                vmem((BATCH, 2, WIDTH), BF16),
                vmem((BATCH, 2, PAGE, WIDTH), BF16),
                vmem((BATCH, PAGE, 2 * ROPE), BF16),
                vmem((SLOTS, 8, 2, PAGE, LATENT), BF16),
                vmem((3, 8, 3, PAGE, 2 * ROPE), BF16),
                vmem((3, 8, 4, QW), BF16),
                vmem((3, 8, 4, QW), BF16),
                vmem((3, 3, 4, 4, 8, QW), BF16),
                vmem((3, 3, 4, 4, 16, LATENT), BF16),
                vmem((SLOTS, 4, 4, 16, LATENT), BF16),
                vmem((3, 3, 4, 16, LATENT), BF16),
                vmem((SLOTS, 4, 16, LATENT), BF16),
                vmem((3, 3, 4, 16, 128), BF16),
                vmem((SLOTS, 4, 16, 128), BF16),
                vmem((3, 4, 16, 128), BF16),
                vmem((3, 4, 16, 128), BF16),
                vmem((51, 16, 128), BF16),
                vmem((3, 8, 8, LATENT), BF16),
                vmem((3, 8, 8, LATENT), BF16),
                dma, dma, dma,
                dma, dma((SLOTS,)), dma,
                dma, dma,
                dma, dma,
                dma, dma((3,)),
                dma, dma((3, 2)),
                dma, dma((3,)),
                dma, dma((SLOTS,)),
                dma, dma((3,)),
                dma, dma,
                dma, dma,
            ],
            compiler_params=pltpu.CompilerParams(collective_id=0, has_side_effects=True, vmem_limit_bytes=44 * 1024 * 1024),
            name='mla',
        )(hbm(len_blk), hbm(q_blk.reshape(BATCH, 2, WIDTH)), kv_blk)
        return out.reshape(BATCH, 2, 1, LATENT)

    return jax.shard_map(local_step, mesh=mesh, in_specs=(P('dp', None, 'dcp', None), P('dp', None, 'dcp', None, None), P('dp')), out_specs=P('dp', None, 'dcp', None), check_vma=False)
```

```python
import jax
import jax.numpy as jnp
from jax import lax
from jax.experimental import pallas as pl
from jax.experimental.pallas import tpu as pltpu
from jax.sharding import PartitionSpec as P

LATENT = 512
ROPE = 64
NOPE = 128
WIDTH = LATENT + ROPE
QW = 2 * LATENT + 2 * ROPE
PAGE = 64
GROUP = 128
BATCH = 64
MASKED = -1e30
SCALE = (NOPE + ROPE) ** -0.5
MESH = pl.DeviceIdType.MESH
BF16 = jnp.bfloat16
F32 = jnp.float32

SZ, SY, SX = 32, 8, 2
RING = (SZ, SY, SX)
BIG = (SX, SZ, SY)
SMALL = (SY, SX, SZ)
COUNT = (3, 3, 2)
BASE = (0, 24, 48)
SLOTS = 8
STEPS = (1, 3, 2)
SENDS = (2, 1, 3)
UNITS = ((0, 0, 3, True), (1, 0, 3, False), (2, 0, 2, True))


def pick(k, vals):
    return jnp.where(k == 0, vals[0], jnp.where(k == 1, vals[1], vals[2]))


def coord(me, stride):
    return lax.rem(lax.div(me, stride), 4)


def shifted(me, stride, d):
    c = coord(me, stride)
    return me + (lax.rem(c + d, 4) - c) * stride


def remote(src, dst, ssem, rsem, dev):
    return pltpu.make_async_remote_copy(src_ref=src, dst_ref=dst, send_sem=ssem, recv_sem=rsem, device_id={'dcp': dev}, device_id_type=MESH)


def arrived(view, sem):
    pltpu.make_async_copy(view, view, sem).wait()


def split3(v):
    hi = v.astype(BF16).astype(F32)
    mid = (v - hi).astype(BF16).astype(F32)
    return hi, mid, v - hi - mid


def put_lse(tile, lse, b):
    lane = lax.broadcasted_iota(jnp.int32, tile.shape, len(tile.shape) - 1)
    for j, v in enumerate(split3(lse)):
        tile = jnp.where(lane == 32 * b + j, v, tile)
    return tile


def get_lse(x, b):
    return sum(x[..., 32 * b + j:32 * b + j + 1] for j in range(3))


def tile_lse(lse):
    tile = jnp.zeros((4, 16, 128), F32)
    for b in range(4):
        tile = put_lse(tile, lse[:, b], b)
    return tile.astype(BF16)


def untile_lse(x):
    return jnp.stack([get_lse(x, b) for b in range(4)], axis=1)


def first(count):
    return pl.ds(0, count)


def onehot(shape, fn):
    row = lax.broadcasted_iota(jnp.int32, shape, 0)
    col = lax.broadcasted_iota(jnp.int32, shape, 1)
    return jnp.where(fn(row, col), 1.0, 0.0).astype(BF16)


def by_set(rows, cols, pad, tokens, tok):
    hit = None
    for k in range(3):
        n = COUNT[k]
        r = rows - k * 8 * pad
        o, j = lax.div(jnp.maximum(r, 0), pad), r & (pad - 1)
        m = (r >= 0) & (r < 8 * pad) & (j < n * tokens) & (cols == 2 * (BASE[k] + o * n) + (2 // tokens) * j + tok)
        hit = m if hit is None else hit | m
    return hit


def kernel(len_hbm, q_ref, kv_ref, out_ref, len_ref, qlocal, kvlocal, ropes, kvbuf, kvrope, qsend, q0buf, qbuf, obuf, r1buf, m1buf, r2buf,
           l1send, l1recv, l2send, l2recv, tally, fsend, frecv,
           len_s, ql_s, loc_s, kv_s, kv_r, kv_l, kr_s, kr_r, q0_s, q0_r, q1_s, q1_r, q2_s, q2_r, q3_s, q3_r, r1_s, r1_r, r2_s, r2_r,
           l1_s, l2_s, f_s, f_r):
    me = lax.axis_index('dcp')
    core = lax.rem(me, 2)
    queries = pltpu.make_async_copy(q_ref, qlocal, ql_s)
    queries.start()
    lens = pltpu.make_async_copy(len_hbm, len_ref, len_s)
    lens.start()
    local = pltpu.make_async_copy(kv_ref.at[:, :, 0], kvlocal, loc_s)
    local.start()

    bar = pltpu.get_barrier_semaphore()
    peers = [me + 1 - 2 * core]
    for s in (SZ, SY, SX):
        for d in STEPS:
            t = shifted(me, s, d)
            peers += [t, t + 1 - 2 * core]
    for t in peers:
        pl.semaphore_signal(bar, inc=1, device_id={'dcp': t}, device_id_type=MESH)
    perms = [onehot((96, 128), lambda r, c, tok=tok: by_set(r, c, 4, 1, tok)) for tok in range(2)]
    queries.wait()
    both = [jnp.dot(perm, qlocal[...].reshape(2 * BATCH, WIDTH), preferred_element_type=F32).astype(BF16) for perm in perms]
    for tok in range(2):
        qsend[:, :, :, pl.ds(tok * LATENT, LATENT)] = both[tok][:, :LATENT].reshape(3, 8, 4, LATENT)
    rotary = jnp.concatenate([both[0][:, LATENT:], both[1][:, LATENT:]], axis=1)
    qsend[:, :, :, pl.ds(2 * LATENT, 2 * ROPE)] = rotary.reshape(3, 8, 4, 2 * ROPE)
    pl.semaphore_wait(bar, len(peers))
    own = [coord(me, RING[k]) * 2 + core for k in range(3)]

    def ring_dest(k, d, flip):
        dev = shifted(me, RING[k], d)
        dcore = core
        if flip:
            dev = dev + 1 - 2 * core
            dcore = 1 - core
        return dev, coord(dev, RING[k]) * 2 + dcore

    near = [(d, flip) for flip in range(2) for d in STEPS[:2]]
    far = [(STEPS[2], flip) for flip in range(2)] + [(0, 1)]
    others = near + far

    for k in range(3):
        for d, flip in others:
            dev, o = ring_dest(k, d, flip)
            remote(qsend.at[k, o], q0buf.at[k, own[k]], q0_s, q0_r, dev).start()
        q0buf[k, own[k]] = qsend[k, own[k]]

    def latent(b):
        return kv_ref.at[b, :, 0, :, first(LATENT)]

    def send_cache(t, which):
        k, i = t % 3, t // 3
        for d, flip in which:
            dev, o = ring_dest(k, d, flip)
            remote(latent(BASE[k] + o * COUNT[k] + i), kvbuf.at[t, own[k]], kv_s, kv_r.at[t], dev).start()
    for t in range(3):
        send_cache(t, near)
    send_cache(2, far)
    big = [coord(me, BIG[k]) for k in range(3)]
    small = [coord(me, SMALL[k]) for k in range(3)]
    arrived(q0buf.at[:, first(7)], q0_r)
    for k in range(3):
        n = COUNT[k]
        order = onehot((n * 8, 32), lambda r, c: c == ((r & 7) << 2) + (r >> 3))
        piece = jnp.dot(order, q0buf[k].reshape(32, QW), preferred_element_type=F32).astype(BF16)
        qbuf[k, first(n), big[k], small[k]] = piece.reshape(n, 8, QW)
    for j, (k, i, n, last_big) in enumerate(UNITS):
        view = qbuf.at[k, pl.ds(i, n), big[k], small[k]]
        for d in STEPS:
            dev = shifted(me, SMALL[k] if last_big else BIG[k], d)
            remote(view, view, q1_s, q1_r.at[j], dev).start()
    for t in range(2):
        send_cache(t, far)

    def block(u, idx, lo, cnt):
        k, i, n, last_big = UNITS[u]
        if last_big:
            return qbuf.at[k, pl.ds(i, n), idx, pl.ds(lo, cnt)]
        return qbuf.at[k, pl.ds(i, n), pl.ds(lo, cnt), idx]

    mid = [big[k] if last_big else small[k] for k, i, n, last_big in UNITS]
    axis = [BIG[k] if last_big else SMALL[k] for k, i, n, last_big in UNITS]
    for u in range(3):
        arrived(block(u, 0, 0, 3), q1_r.at[u])
        view = block(u, mid[u], 0, 4)
        for j, d in enumerate(STEPS[:2]):
            remote(view, view, q2_s, q2_r.at[u, j], shifted(me, axis[u], d)).start()
    local.wait()
    def pack(b, carry):
        ropes[b] = jnp.concatenate([kvlocal[b, 0, :, pl.ds(LATENT, ROPE)], kvlocal[b, 1, :, pl.ds(LATENT, ROPE)]], axis=1)
        return carry

    lax.fori_loop(0, BATCH, pack, 0, unroll=4)
    for k in range(3):
        n = COUNT[k]
        for d, flip in others:
            dev, o = ring_dest(k, d, flip)
            remote(ropes.at[pl.ds(BASE[k] + o * n, n)], kvrope.at[k, own[k], first(n)], kr_s, kr_r, dev).start()
        kvrope[k, own[k], first(n)] = ropes[pl.ds(BASE[k] + own[k] * n, n)]

    send_cache(3, others)
    send_cache(4, others[:2])
    send_cache(5, others[:2])

    def forward(k):
        for j, d in enumerate(STEPS[:2]):
            arrived(block(k, mid[k], 0, 4), q2_r.at[k, j])
            half = block(k, lax.rem(mid[k] + (3 if j == 0 else 1), 4), 2 * j, 2)
            remote(half, half, q3_s, q3_r.at[k], shifted(me, axis[k], d)).start()
    forward(2)
    send_cache(4, others[2:])
    send_cache(6, others)
    send_cache(7, others)
    forward(0)
    forward(1)
    send_cache(5, others[2:])
    for t in range(SLOTS):
        k, i = t % 3, t // 3
        pltpu.make_async_copy(latent(BASE[k] + own[k] * COUNT[k] + i), kvbuf.at[t, own[k]], kv_l).start()

    lens.wait()
    arrived(ropes.at[first(56)], kr_r)
    arrived(kvbuf.at[:, 0], kv_l)
    def attend(t, carry):
        k = lax.rem(t, 3)
        i = lax.div(t, 3)
        ring = pick(k, RING)
        u = coord(me, ring)
        bstride = pick(k, BIG)
        b_me = coord(me, bstride)
        length = len_ref[24 * k + (u * 2 + core) * pick(k, COUNT) + i]
        for unit in range(3):

            @pl.when(t == unit)
            def _():
                arrived(block(unit, 0, 0, 4), q3_r.at[unit])
        arrived(kvbuf.at[t, first(7)], kv_r.at[t])
        q2 = qbuf[k, i].reshape(128, QW)
        q = jnp.concatenate([q2[:, :LATENT], q2[:, LATENT:2 * LATENT]], axis=0)
        pair = q2[:, 2 * LATENT:]
        swapped = jnp.concatenate([pair[:, ROPE:], pair[:, :ROPE]], axis=1)
        low = lax.broadcasted_iota(jnp.int32, pair.shape, 1) < ROPE
        qr = jnp.concatenate([jnp.where(low, pair, swapped), jnp.where(low, swapped, pair)], axis=0)
        keys = kvbuf[t].reshape(1024, LATENT)
        packed = kvrope[k, :, i]
        lane = lax.broadcasted_iota(jnp.int32, packed.shape, 2)
        zero = jnp.zeros_like(packed)
        rope = jnp.stack([jnp.where(lane < ROPE, packed, zero), jnp.where(lane >= ROPE, packed, zero)], axis=1).reshape(1024, 2 * ROPE)
        nt = (((1,), (1,)), ((), ()))
        s = lax.dot_general(jnp.concatenate([q, qr], axis=1), jnp.concatenate([keys, rope], axis=1), nt, preferred_element_type=F32)
        s = s * SCALE
        kk = lax.broadcasted_iota(jnp.int32, (1, 1024), 1)
        dsrc = (me - u * ring - core) + (kk >> 8) * ring + ((kk >> 7) & 1)
        pos = (((kk >> 6) & 1) * GROUP + dsrc) * PAGE + (kk & 63)
        tok = lax.broadcasted_iota(jnp.int32, (256, 1), 0) >> 7
        s = jnp.where(pos - tok <= length - 2, s, MASKED)
        m = jnp.max(s, axis=1, keepdims=True)
        w = jnp.exp(s - m)
        l = jnp.sum(w, axis=1, keepdims=True)
        part = jnp.dot(w.astype(BF16), keys, preferred_element_type=F32)
        part = (part * (1.0 / l)).astype(BF16)
        obuf[k, i, :, :, first(8)] = part[:128].reshape(4, 4, 8, LATENT)
        obuf[k, i, :, :, pl.ds(8, 8)] = part[128:].reshape(4, 4, 8, LATENT)
        lse = m + jnp.log(l)
        l1send[k, i] = tile_lse(jnp.concatenate([lse[:128].reshape(4, 4, 8, 1), lse[128:].reshape(4, 4, 8, 1)], axis=2))
        for d in SENDS:
            b = lax.rem(b_me + d, 4)
            dev = me + (b - b_me) * bstride
            remote(obuf.at[k, i, b], r1buf.at[t, b_me], r1_s, r1_r.at[t], dev).start()
            remote(l1send.at[k, i, b], l1recv.at[t, b_me], l1_s, r1_r.at[t], dev).start()
        r1buf[t, b_me] = obuf[k, i, b_me]
        l1recv[t, b_me] = l1send[k, i, b_me]
        return carry

    lax.fori_loop(0, SLOTS, attend, 0)

    def merge(lse, ref):
        top = jnp.max(lse, axis=0)
        e = jnp.exp(lse - top[None])
        total = jnp.sum(e, axis=0)
        wgt = e / total[None]
        acc = wgt[0] * ref[0].astype(F32)
        for p in range(1, ref.shape[0]):
            acc = acc + wgt[p] * ref[p].astype(F32)
        return acc.astype(BF16), top + jnp.log(total)

    lacc = [jnp.zeros((4, 16, 128), F32) for _ in range(3)]
    for t in (0, 1, 3, 4, 2, 6, 5, 7):
        k, i = t % 3, t // 3
        arrived(tally.at[first(51)], r1_r.at[t])
        both, lse = merge(untile_lse(l1recv[t].astype(F32)), r1buf.at[t])
        m1buf[k, i] = both
        lacc[k] = put_lse(lacc[k], lse, i)
        for d in SENDS:
            b = lax.rem(small[k] + d, 4)
            remote(m1buf.at[k, i, b], r2buf.at[t, small[k]], r2_s, r2_r.at[k], shifted(me, SMALL[k], d)).start()
        r2buf[t, small[k]] = m1buf[k, i, small[k]]
        if i == COUNT[k] - 1:
            l2send[k] = lacc[k].astype(BF16)
            for d in SENDS:
                b = lax.rem(small[k] + d, 4)
                remote(l2send.at[k, b], l2recv.at[k, small[k]], l2_s, r2_r.at[k], shifted(me, SMALL[k], d)).start()
            l2recv[k, small[k]] = l2send[k, small[k]]

    for k in (0, 2, 1):
        n = COUNT[k]
        arrived(tally.at[first(12 * n + 3)], r2_r.at[k])
        lr = l2recv[k].astype(F32)
        merged = []
        for i in range(n):
            t = 3 * i + k
            merged.append(merge(get_lse(lr, i), r2buf.at[t])[0])
        order = onehot((64, n * 16), lambda r, c: r == ((c & 7) << 3) + ((c >> 4) << 1) + ((c >> 3) & 1))
        out = jnp.dot(order, jnp.concatenate(merged, axis=0), preferred_element_type=F32)
        fsend[k] = out.astype(BF16).reshape(8, 8, LATENT)
        for d, flip in far + near:
            dev, o = ring_dest(k, d, flip)
            remote(fsend.at[k, o], frecv.at[k, own[k]], f_s, f_r, dev).start()
        frecv[k, own[k]] = fsend[k, own[k]]
    back = onehot((128, 192), lambda r, c: by_set(c, r, 8, 2, 0))
    arrived(frecv.at[:, first(7)], f_r)
    out = jnp.dot(back, frecv[...].reshape(192, LATENT), preferred_element_type=F32)
    out_ref[...] = out.astype(BF16).reshape(BATCH, 2, LATENT)
    def sent(view, sem):
        remote(view, view, sem, sem, me).wait_send()

    sent(q0buf.at[:, first(7)], q0_s)
    sent(qbuf.at[first(2), :, :, 0], q1_s)
    sent(qbuf.at[first(2), first(2)], q2_s)
    sent(qbuf.at[first(2), 0], q3_s)
    sent(ropes.at[first(56)], kr_s)
    sent(kvbuf.at[:, first(7)], kv_s)
    sent(r1buf.at[first(SLOTS), first(3)], r1_s)
    sent(l1recv.at[first(SLOTS), first(3)], l1_s)
    sent(r2buf.at[first(SLOTS), first(3)], r2_s)
    sent(l2recv.at[:, first(3)], l2_s)
    sent(frecv.at[:, first(7)], f_s)


def solution(mesh):
    def local_step(q_blk, kv_blk, len_blk):
        dma = pltpu.SemaphoreType.DMA
        vmem = pltpu.VMEM

        def hbm(v):
            return pltpu.with_memory_space_constraint(v, pltpu.HBM)

        out = pl.pallas_call(
            kernel,
            out_shape=jax.ShapeDtypeStruct((BATCH, 2, LATENT), BF16),
            in_specs=[
                pl.BlockSpec(memory_space=pltpu.HBM),
                pl.BlockSpec(memory_space=pltpu.HBM),
                pl.BlockSpec(memory_space=pltpu.HBM),
            ],
            out_specs=pl.BlockSpec(memory_space=pltpu.VMEM),
            scratch_shapes=[
                pltpu.SMEM((BATCH,), jnp.int32),
                vmem((BATCH, 2, WIDTH), BF16),
                vmem((BATCH, 2, PAGE, WIDTH), BF16),
                vmem((BATCH, PAGE, 2 * ROPE), BF16),
                vmem((SLOTS, 8, 2, PAGE, LATENT), BF16),
                vmem((3, 8, 3, PAGE, 2 * ROPE), BF16),
                vmem((3, 8, 4, QW), BF16),
                vmem((3, 8, 4, QW), BF16),
                vmem((3, 3, 4, 4, 8, QW), BF16),
                vmem((3, 3, 4, 4, 16, LATENT), BF16),
                vmem((SLOTS, 4, 4, 16, LATENT), BF16),
                vmem((3, 3, 4, 16, LATENT), BF16),
                vmem((SLOTS, 4, 16, LATENT), BF16),
                vmem((3, 3, 4, 16, 128), BF16),
                vmem((SLOTS, 4, 16, 128), BF16),
                vmem((3, 4, 16, 128), BF16),
                vmem((3, 4, 16, 128), BF16),
                vmem((51, 16, 128), BF16),
                vmem((3, 8, 8, LATENT), BF16),
                vmem((3, 8, 8, LATENT), BF16),
                dma, dma, dma,
                dma, dma((SLOTS,)), dma,
                dma, dma,
                dma, dma,
                dma, dma((3,)),
                dma, dma((3, 2)),
                dma, dma((3,)),
                dma, dma((SLOTS,)),
                dma, dma((3,)),
                dma, dma,
                dma, dma,
            ],
            compiler_params=pltpu.CompilerParams(collective_id=0, has_side_effects=True, vmem_limit_bytes=44 * 1024 * 1024),
            name='mla',
        )(hbm(len_blk), hbm(q_blk.reshape(BATCH, 2, WIDTH)), kv_blk)
        return out.reshape(BATCH, 2, 1, LATENT)

    return jax.shard_map(local_step, mesh=mesh, in_specs=(P('dp', None, 'dcp', None), P('dp', None, 'dcp', None, None), P('dp')), out_specs=P('dp', None, 'dcp', None), check_vma=False)
```

```python
import jax
import jax.numpy as jnp
from jax import lax
from jax.experimental import pallas as pl
from jax.experimental.pallas import tpu as pltpu
from jax.sharding import PartitionSpec as P

LATENT = 512
ROPE = 64
NOPE = 128
WIDTH = LATENT + ROPE
QW = 2 * LATENT + 2 * ROPE
PAGE = 64
GROUP = 128
BATCH = 64
MASKED = -1e30
SCALE = (NOPE + ROPE) ** -0.5
MESH = pl.DeviceIdType.MESH
BF16 = jnp.bfloat16
F32 = jnp.float32

SZ, SY, SX = 32, 8, 2
RING = (SZ, SY, SX)
BIG = (SX, SZ, SY)
SMALL = (SY, SX, SZ)
COUNT = (3, 3, 2)
BASE = (0, 24, 48)
SLOTS = 8
STEPS = (1, 3, 2)
SENDS = (2, 1, 3)
UNITS = ((0, 0, 3, True), (1, 0, 3, False), (2, 0, 2, True))


def pick(k, vals):
    return jnp.where(k == 0, vals[0], jnp.where(k == 1, vals[1], vals[2]))


def coord(me, stride):
    return lax.rem(lax.div(me, stride), 4)


def shifted(me, stride, d):
    c = coord(me, stride)
    return me + (lax.rem(c + d, 4) - c) * stride


def remote(src, dst, ssem, rsem, dev):
    return pltpu.make_async_remote_copy(src_ref=src, dst_ref=dst, send_sem=ssem, recv_sem=rsem, device_id={'dcp': dev}, device_id_type=MESH)


def arrived(view, sem):
    pltpu.make_async_copy(view, view, sem).wait()


def split3(v):
    hi = v.astype(BF16).astype(F32)
    mid = (v - hi).astype(BF16).astype(F32)
    return hi, mid, v - hi - mid


def put_lse(tile, lse, b):
    lane = lax.broadcasted_iota(jnp.int32, tile.shape, len(tile.shape) - 1)
    for j, v in enumerate(split3(lse)):
        tile = jnp.where(lane == 32 * b + j, v, tile)
    return tile


def get_lse(x, b):
    return sum(x[..., 32 * b + j:32 * b + j + 1] for j in range(3))


def tile_lse(lse):
    tile = jnp.zeros((4, 16, 128), F32)
    for b in range(4):
        tile = put_lse(tile, lse[:, b], b)
    return tile.astype(BF16)


def untile_lse(x):
    return jnp.stack([get_lse(x, b) for b in range(4)], axis=1)


def first(count):
    return pl.ds(0, count)


def onehot(shape, fn):
    row = lax.broadcasted_iota(jnp.int32, shape, 0)
    col = lax.broadcasted_iota(jnp.int32, shape, 1)
    return jnp.where(fn(row, col), 1.0, 0.0).astype(BF16)


def by_set(rows, cols, pad, tokens, tok):
    hit = None
    for k in range(3):
        n = COUNT[k]
        r = rows - k * 8 * pad
        o, j = lax.div(jnp.maximum(r, 0), pad), r & (pad - 1)
        m = (r >= 0) & (r < 8 * pad) & (j < n * tokens) & (cols == 2 * (BASE[k] + o * n) + (2 // tokens) * j + tok)
        hit = m if hit is None else hit | m
    return hit


def kernel(len_hbm, q_ref, kv_ref, out_ref, len_ref, qlocal, kvlocal, ropes, kvbuf, kvrope, qsend, q0buf, qbuf, obuf, r1buf, m1buf, r2buf,
           l1send, l1recv, l2send, l2recv, tally, fsend, frecv,
           all_s,
           len_s, ql_s, loc_s, kv_s, kv_r, kv_l, kr_r, q0_s, q0_r, q1_r, q2_r, q3_r, r1_r, r2_r,
           f_r):
    me = lax.axis_index('dcp')
    core = lax.rem(me, 2)
    queries = pltpu.make_async_copy(q_ref, qlocal, ql_s)
    queries.start()
    lens = pltpu.make_async_copy(len_hbm, len_ref, len_s)
    lens.start()
    local = pltpu.make_async_copy(kv_ref.at[:, :, 0], kvlocal, loc_s)
    local.start()

    bar = pltpu.get_barrier_semaphore()
    peers = [me + 1 - 2 * core]
    for s in (SZ, SY, SX):
        for d in STEPS:
            t = shifted(me, s, d)
            peers += [t, t + 1 - 2 * core]
    for t in peers:
        pl.semaphore_signal(bar, inc=1, device_id={'dcp': t}, device_id_type=MESH)
    perms = [onehot((96, 128), lambda r, c, tok=tok: by_set(r, c, 4, 1, tok)) for tok in range(2)]
    queries.wait()
    both = [jnp.dot(perm, qlocal[...].reshape(2 * BATCH, WIDTH), preferred_element_type=F32).astype(BF16) for perm in perms]
    for tok in range(2):
        qsend[:, :, :, pl.ds(tok * LATENT, LATENT)] = both[tok][:, :LATENT].reshape(3, 8, 4, LATENT)
    rotary = jnp.concatenate([both[0][:, LATENT:], both[1][:, LATENT:]], axis=1)
    qsend[:, :, :, pl.ds(2 * LATENT, 2 * ROPE)] = rotary.reshape(3, 8, 4, 2 * ROPE)
    pl.semaphore_wait(bar, len(peers))
    own = [coord(me, RING[k]) * 2 + core for k in range(3)]

    def ring_dest(k, d, flip):
        dev = shifted(me, RING[k], d)
        dcore = core
        if flip:
            dev = dev + 1 - 2 * core
            dcore = 1 - core
        return dev, coord(dev, RING[k]) * 2 + dcore

    near = [(d, flip) for flip in range(2) for d in STEPS[:2]]
    far = [(STEPS[2], flip) for flip in range(2)] + [(0, 1)]
    others = near + far

    for k in range(3):
        for d, flip in others:
            dev, o = ring_dest(k, d, flip)
            remote(qsend.at[k, o], q0buf.at[k, own[k]], q0_s, q0_r, dev).start()
        q0buf[k, own[k]] = qsend[k, own[k]]

    def latent(b):
        return kv_ref.at[b, :, 0, :, first(LATENT)]

    def send_cache(t, which):
        k, i = t % 3, t // 3
        for d, flip in which:
            dev, o = ring_dest(k, d, flip)
            remote(latent(BASE[k] + o * COUNT[k] + i), kvbuf.at[t, own[k]], kv_s, kv_r.at[t], dev).start()
    for t in range(3):
        send_cache(t, near)
    send_cache(2, far)
    big = [coord(me, BIG[k]) for k in range(3)]
    small = [coord(me, SMALL[k]) for k in range(3)]
    arrived(q0buf.at[:, first(7)], q0_r)
    for k in range(3):
        n = COUNT[k]
        order = onehot((n * 8, 32), lambda r, c: c == ((r & 7) << 2) + (r >> 3))
        piece = jnp.dot(order, q0buf[k].reshape(32, QW), preferred_element_type=F32).astype(BF16)
        qbuf[k, first(n), big[k], small[k]] = piece.reshape(n, 8, QW)
    for j, (k, i, n, last_big) in enumerate(UNITS):
        view = qbuf.at[k, pl.ds(i, n), big[k], small[k]]
        for d in STEPS:
            dev = shifted(me, SMALL[k] if last_big else BIG[k], d)
            remote(view, view, all_s, q1_r.at[j], dev).start()
    for t in range(2):
        send_cache(t, far)

    def block(u, idx, lo, cnt):
        k, i, n, last_big = UNITS[u]
        if last_big:
            return qbuf.at[k, pl.ds(i, n), idx, pl.ds(lo, cnt)]
        return qbuf.at[k, pl.ds(i, n), pl.ds(lo, cnt), idx]

    mid = [big[k] if last_big else small[k] for k, i, n, last_big in UNITS]
    axis = [BIG[k] if last_big else SMALL[k] for k, i, n, last_big in UNITS]
    for u in range(3):
        arrived(block(u, 0, 0, 3), q1_r.at[u])
        view = block(u, mid[u], 0, 4)
        for j, d in enumerate(STEPS[:2]):
            remote(view, view, all_s, q2_r.at[u, j], shifted(me, axis[u], d)).start()
    local.wait()
    def pack(b, carry):
        ropes[b] = jnp.concatenate([kvlocal[b, 0, :, pl.ds(LATENT, ROPE)], kvlocal[b, 1, :, pl.ds(LATENT, ROPE)]], axis=1)
        return carry

    lax.fori_loop(0, BATCH, pack, 0, unroll=4)
    for k in range(3):
        n = COUNT[k]
        for d, flip in others:
            dev, o = ring_dest(k, d, flip)
            remote(ropes.at[pl.ds(BASE[k] + o * n, n)], kvrope.at[k, own[k], first(n)], all_s, kr_r, dev).start()
        kvrope[k, own[k], first(n)] = ropes[pl.ds(BASE[k] + own[k] * n, n)]

    send_cache(3, others)
    send_cache(4, others[:2])
    send_cache(5, others[:2])

    def forward(k):
        for j, d in enumerate(STEPS[:2]):
            arrived(block(k, mid[k], 0, 4), q2_r.at[k, j])
            half = block(k, lax.rem(mid[k] + (3 if j == 0 else 1), 4), 2 * j, 2)
            remote(half, half, all_s, q3_r.at[k], shifted(me, axis[k], d)).start()
    forward(2)
    send_cache(4, others[2:])
    send_cache(6, others)
    send_cache(7, others)
    forward(0)
    forward(1)
    send_cache(5, others[2:])
    for t in range(SLOTS):
        k, i = t % 3, t // 3
        pltpu.make_async_copy(latent(BASE[k] + own[k] * COUNT[k] + i), kvbuf.at[t, own[k]], kv_l).start()

    lens.wait()
    arrived(ropes.at[first(56)], kr_r)
    arrived(kvbuf.at[:, 0], kv_l)
    def attend(t, carry):
        k = lax.rem(t, 3)
        i = lax.div(t, 3)
        ring = pick(k, RING)
        u = coord(me, ring)
        bstride = pick(k, BIG)
        b_me = coord(me, bstride)
        length = len_ref[24 * k + (u * 2 + core) * pick(k, COUNT) + i]
        for unit in range(3):

            @pl.when(t == unit)
            def _():
                arrived(block(unit, 0, 0, 4), q3_r.at[unit])
        arrived(kvbuf.at[t, first(7)], kv_r.at[t])
        q2 = qbuf[k, i].reshape(128, QW)
        q = jnp.concatenate([q2[:, :LATENT], q2[:, LATENT:2 * LATENT]], axis=0)
        pair = q2[:, 2 * LATENT:]
        swapped = jnp.concatenate([pair[:, ROPE:], pair[:, :ROPE]], axis=1)
        low = lax.broadcasted_iota(jnp.int32, pair.shape, 1) < ROPE
        qr = jnp.concatenate([jnp.where(low, pair, swapped), jnp.where(low, swapped, pair)], axis=0)
        keys = kvbuf[t].reshape(1024, LATENT)
        packed = kvrope[k, :, i]
        lane = lax.broadcasted_iota(jnp.int32, packed.shape, 2)
        zero = jnp.zeros_like(packed)
        rope = jnp.stack([jnp.where(lane < ROPE, packed, zero), jnp.where(lane >= ROPE, packed, zero)], axis=1).reshape(1024, 2 * ROPE)
        nt = (((1,), (1,)), ((), ()))
        s = lax.dot_general(jnp.concatenate([q, qr], axis=1), jnp.concatenate([keys, rope], axis=1), nt, preferred_element_type=F32)
        s = s * SCALE
        kk = lax.broadcasted_iota(jnp.int32, (1, 1024), 1)
        dsrc = (me - u * ring - core) + (kk >> 8) * ring + ((kk >> 7) & 1)
        pos = (((kk >> 6) & 1) * GROUP + dsrc) * PAGE + (kk & 63)
        tok = lax.broadcasted_iota(jnp.int32, (256, 1), 0) >> 7
        s = jnp.where(pos - tok <= length - 2, s, MASKED)
        m = jnp.max(s, axis=1, keepdims=True)
        w = jnp.exp(s - m)
        l = jnp.sum(w, axis=1, keepdims=True)
        part = jnp.dot(w.astype(BF16), keys, preferred_element_type=F32)
        part = (part * (1.0 / l)).astype(BF16)
        obuf[k, i, :, :, first(8)] = part[:128].reshape(4, 4, 8, LATENT)
        obuf[k, i, :, :, pl.ds(8, 8)] = part[128:].reshape(4, 4, 8, LATENT)
        lse = m + jnp.log(l)
        l1send[k, i] = tile_lse(jnp.concatenate([lse[:128].reshape(4, 4, 8, 1), lse[128:].reshape(4, 4, 8, 1)], axis=2))
        for d in SENDS:
            b = lax.rem(b_me + d, 4)
            dev = me + (b - b_me) * bstride
            remote(obuf.at[k, i, b], r1buf.at[t, b_me], all_s, r1_r.at[t], dev).start()
            remote(l1send.at[k, i, b], l1recv.at[t, b_me], all_s, r1_r.at[t], dev).start()
        r1buf[t, b_me] = obuf[k, i, b_me]
        l1recv[t, b_me] = l1send[k, i, b_me]
        return carry

    lax.fori_loop(0, SLOTS, attend, 0)

    def merge(lse, ref):
        top = jnp.max(lse, axis=0)
        e = jnp.exp(lse - top[None])
        total = jnp.sum(e, axis=0)
        wgt = e / total[None]
        acc = wgt[0] * ref[0].astype(F32)
        for p in range(1, ref.shape[0]):
            acc = acc + wgt[p] * ref[p].astype(F32)
        return acc.astype(BF16), top + jnp.log(total)

    lacc = [jnp.zeros((4, 16, 128), F32) for _ in range(3)]
    for t in (0, 1, 3, 4, 2, 6, 5, 7):
        k, i = t % 3, t // 3
        arrived(tally.at[first(51)], r1_r.at[t])
        both, lse = merge(untile_lse(l1recv[t].astype(F32)), r1buf.at[t])
        m1buf[k, i] = both
        lacc[k] = put_lse(lacc[k], lse, i)
        for d in SENDS:
            b = lax.rem(small[k] + d, 4)
            remote(m1buf.at[k, i, b], r2buf.at[t, small[k]], all_s, r2_r.at[k], shifted(me, SMALL[k], d)).start()
        r2buf[t, small[k]] = m1buf[k, i, small[k]]
        if i == COUNT[k] - 1:
            l2send[k] = lacc[k].astype(BF16)
            for d in SENDS:
                b = lax.rem(small[k] + d, 4)
                remote(l2send.at[k, b], l2recv.at[k, small[k]], all_s, r2_r.at[k], shifted(me, SMALL[k], d)).start()
            l2recv[k, small[k]] = l2send[k, small[k]]

    for k in (0, 2, 1):
        n = COUNT[k]
        arrived(tally.at[first(12 * n + 3)], r2_r.at[k])
        lr = l2recv[k].astype(F32)
        merged = []
        for i in range(n):
            t = 3 * i + k
            merged.append(merge(get_lse(lr, i), r2buf.at[t])[0])
        order = onehot((64, n * 16), lambda r, c: r == ((c & 7) << 3) + ((c >> 4) << 1) + ((c >> 3) & 1))
        out = jnp.dot(order, jnp.concatenate(merged, axis=0), preferred_element_type=F32)
        fsend[k] = out.astype(BF16).reshape(8, 8, LATENT)
        for d, flip in far + near:
            dev, o = ring_dest(k, d, flip)
            remote(fsend.at[k, o], frecv.at[k, own[k]], all_s, f_r, dev).start()
        frecv[k, own[k]] = fsend[k, own[k]]
    back = onehot((128, 192), lambda r, c: by_set(c, r, 8, 2, 0))
    arrived(frecv.at[:, first(7)], f_r)
    out = jnp.dot(back, frecv[...].reshape(192, LATENT), preferred_element_type=F32)
    out_ref[...] = out.astype(BF16).reshape(BATCH, 2, LATENT)
    def sent(view, sem):
        remote(view, view, sem, sem, me).wait_send()

    sent(tally, all_s)
    sent(q0buf.at[:, first(7)], q0_s)
    sent(kvbuf.at[:, first(7)], kv_s)


def solution(mesh):
    def local_step(q_blk, kv_blk, len_blk):
        dma = pltpu.SemaphoreType.DMA
        vmem = pltpu.VMEM

        def hbm(v):
            return pltpu.with_memory_space_constraint(v, pltpu.HBM)

        out = pl.pallas_call(
            kernel,
            out_shape=jax.ShapeDtypeStruct((BATCH, 2, LATENT), BF16),
            in_specs=[
                pl.BlockSpec(memory_space=pltpu.HBM),
                pl.BlockSpec(memory_space=pltpu.HBM),
                pl.BlockSpec(memory_space=pltpu.HBM),
            ],
            out_specs=pl.BlockSpec(memory_space=pltpu.VMEM),
            scratch_shapes=[
                pltpu.SMEM((BATCH,), jnp.int32),
                vmem((BATCH, 2, WIDTH), BF16),
                vmem((BATCH, 2, PAGE, WIDTH), BF16),
                vmem((BATCH, PAGE, 2 * ROPE), BF16),
                vmem((SLOTS, 8, 2, PAGE, LATENT), BF16),
                vmem((3, 8, 3, PAGE, 2 * ROPE), BF16),
                vmem((3, 8, 4, QW), BF16),
                vmem((3, 8, 4, QW), BF16),
                vmem((3, 3, 4, 4, 8, QW), BF16),
                vmem((3, 3, 4, 4, 16, LATENT), BF16),
                vmem((SLOTS, 4, 4, 16, LATENT), BF16),
                vmem((3, 3, 4, 16, LATENT), BF16),
                vmem((SLOTS, 4, 16, LATENT), BF16),
                vmem((3, 3, 4, 16, 128), BF16),
                vmem((SLOTS, 4, 16, 128), BF16),
                vmem((3, 4, 16, 128), BF16),
                vmem((3, 4, 16, 128), BF16),
                vmem((1319, 16, 128), BF16),
                vmem((3, 8, 8, LATENT), BF16),
                vmem((3, 8, 8, LATENT), BF16),
                dma,
                dma, dma, dma,
                dma, dma((SLOTS,)), dma,
                dma,
                dma, dma,
                dma((3,)),
                dma((3, 2)),
                dma((3,)),
                dma((SLOTS,)),
                dma((3,)),
                dma,
            ],
            compiler_params=pltpu.CompilerParams(collective_id=0, has_side_effects=True, vmem_limit_bytes=44 * 1024 * 1024),
            name='mla',
        )(hbm(len_blk), hbm(q_blk.reshape(BATCH, 2, WIDTH)), kv_blk)
        return out.reshape(BATCH, 2, 1, LATENT)

    return jax.shard_map(local_step, mesh=mesh, in_specs=(P('dp', None, 'dcp', None), P('dp', None, 'dcp', None, None), P('dp')), out_specs=P('dp', None, 'dcp', None), check_vma=False)
```
